256 devices in a mesh: batch: 8 (over z), rows: 32 (over y, x, core).
Axes of the slice: x: 4, y: 4, z: 8, core: 2. Of those that a mesh axis runs over, the one named last changes fastest.
Arguments:
- level_two: bfloat16 [16, 256, 256, 256], P('batch', 'rows'), parts along dimension 0, may hold values from -130 to 130
- level_three: bfloat16 [16, 128, 128, 512], P('batch', 'rows'), parts along dimension 0, may hold values from -130 to 130
- level_four: bfloat16 [16, 64, 64, 1024], P('batch', 'rows'), parts along dimension 0, may hold values from -130 to 130
- level_five: bfloat16 [16, 32, 32, 2048], P('batch', 'rows'), parts along dimension 0, may hold values from -130 to 130
- lateral_two: bfloat16 [256, 256], replicated, may hold values from -0.375 to 0.375
- lateral_three: bfloat16 [512, 256], replicated, may hold values from -0.25 to 0.25
- lateral_four: bfloat16 [1024, 256], replicated, may hold values from -0.1875 to 0.1875
- lateral_five: bfloat16 [2048, 256], replicated, may hold values from -0.125 to 0.125
- lateral_bias: float32 [4, 256], replicated, may hold values from -4 to 4
- smooth_weight: bfloat16 [4, 3, 768, 256], replicated, may hold values from -0.125 to 0.125
- norm_gain: float32 [4, 256], replicated, may hold values from 0.5 to 1.5
- norm_shift: float32 [4, 256], replicated, may hold values from -2 to 2
Outputs:
- pyramid_two: bfloat16 [16, 256, 256, 256], P('batch', 'rows'), parts along dimension 0
- pyramid_three: bfloat16 [16, 128, 128, 256], P('batch', 'rows'), parts along dimension 0
- pyramid_four: bfloat16 [16, 64, 64, 256], P('batch', 'rows'), parts along dimension 0
- pyramid_five: bfloat16 [16, 32, 32, 256], P('batch', 'rows'), parts along dimension 0
The draws below stay inside these ranges and needn't reach their ends.
There are 8 independent parts, one for each index of `batch`. The reference program is written for one: setup_inputs(seed, part) draws one part's arguments, and reference() takes and returns one part's arrays. A program takes and returns all parts, laid end to end along the dimension named above; an argument that names none is the same for every part. Nothing has to cross between parts.
All inputs are finite; a program needn't handle non-finite values.
Results may differ from the reference program's by a relative error of at most 0.0054.
Values may be sent and summed in bfloat16 or wider, within the bound.
A program may use at most 128 MiB of HBM per device.

```python
import math
import jax
import jax.numpy as jnp
from jax import lax

CHANNELS = 256
DEPTH_TWO = 256
DEPTH_THREE = 512
DEPTH_FOUR = 1024
DEPTH_FIVE = 2048
GROUPS = 32
LEVELS = 4
IMAGES = 2
COLUMNS = 256
HEIGHT = 256


def feature_draw(key, rows_all, cols_all, depth_all, salt_code):
    base_key = jax.random.fold_in(key, salt_code)
    subkeys = jax.random.split(base_key, 3)
    relative = (jnp.arange(rows_all, dtype=jnp.float32) + 0.5) / rows_all
    jitter = jnp.exp(jax.random.uniform(subkeys[0], (IMAGES, rows_all), jnp.float32, 0.0, math.log(3.3)))
    row_scale = jnp.exp(math.log(3.0) * relative)[None, :] * jitter
    chan_scale = jnp.exp(jax.random.uniform(subkeys[1], (depth_all,), jnp.float32, -0.5 * math.log(10.0), 0.5 * math.log(10.0)))
    shape_all = (IMAGES, rows_all, cols_all, depth_all)
    values = jnp.clip(jax.random.normal(subkeys[2], shape_all, jnp.float32), -4.0, 4.0)
    return (values * row_scale[:, :, None, None] * chan_scale).astype(jnp.bfloat16)


def draw_level_two(key, part):
    return feature_draw(key, HEIGHT, COLUMNS, DEPTH_TWO, 11)


def draw_level_three(key, part):
    return feature_draw(key, HEIGHT // 2, COLUMNS // 2, DEPTH_THREE, 12)


def draw_level_four(key, part):
    return feature_draw(key, HEIGHT // 4, COLUMNS // 4, DEPTH_FOUR, 13)


def draw_level_five(key, part):
    return feature_draw(key, HEIGHT // 8, COLUMNS // 8, DEPTH_FIVE, 14)


def bell_draw(rng, shape, width, bound, kind=jnp.bfloat16):
    values = jax.random.normal(rng, shape, jnp.float32) * width
    return jnp.minimum(jnp.maximum(values, -bound), bound).astype(kind)


def setup_inputs(seed: int = 0, part: int = 0) -> dict:
    key_of = jax.random.split(jax.random.key(seed), 13)
    own_keys = jax.random.split(jax.random.fold_in(key_of[12], part), 13)
    return {
        "level_two": draw_level_two(jax.random.fold_in(jax.random.fold_in(key_of[12], part), 71), part),
        "level_three": draw_level_three(jax.random.fold_in(jax.random.fold_in(key_of[12], part), 71), part),
        "level_four": draw_level_four(jax.random.fold_in(jax.random.fold_in(key_of[12], part), 71), part),
        "level_five": draw_level_five(jax.random.fold_in(jax.random.fold_in(key_of[12], part), 71), part),
        "lateral_two": bell_draw(key_of[4], (DEPTH_TWO, CHANNELS), DEPTH_TWO ** -0.5, 0.375),
        "lateral_three": bell_draw(key_of[5], (DEPTH_THREE, CHANNELS), DEPTH_THREE ** -0.5, 0.25),
        "lateral_four": bell_draw(key_of[6], (DEPTH_FOUR, CHANNELS), DEPTH_FOUR ** -0.5, 0.1875),
        "lateral_five": bell_draw(key_of[7], (DEPTH_FIVE, CHANNELS), DEPTH_FIVE ** -0.5, 0.125),
        "lateral_bias": bell_draw(key_of[8], (LEVELS, CHANNELS), 1.0, 4.0, jnp.float32),
        "smooth_weight": bell_draw(key_of[9], (LEVELS, 3, 3 * CHANNELS, CHANNELS), (9 * CHANNELS) ** -0.5, 0.125),
        "norm_gain": jnp.clip(1.0 + 0.1 * jax.random.normal(key_of[10], (LEVELS, CHANNELS), jnp.float32), 0.5, 1.5),
        "norm_shift": bell_draw(key_of[11], (LEVELS, CHANNELS), 0.5, 2.0, jnp.float32),
    }


epsilon = 1e-05

def refine(widened, axis_pos):
    length = widened.shape[axis_pos] - 2
    before = lax.slice_in_dim(widened, 0, length, axis=axis_pos)
    middle = lax.slice_in_dim(widened, 1, length + 1, axis=axis_pos)
    beyond = lax.slice_in_dim(widened, 2, length + 2, axis=axis_pos)
    even_rows = 0.25 * before + 0.75 * middle
    odd_rows = 0.75 * middle + 0.25 * beyond
    stacked = jnp.stack([even_rows, odd_rows], axis_pos + 1)
    new_shape = list(widened.shape)
    new_shape[axis_pos] = 2 * length
    return stacked.reshape(new_shape)

def edge_columns(values):
    return jnp.concatenate([values[:, :, :1], values, values[:, :, -1:]], 2)

def lateral(feature, weight, bias_row):
    flattened = feature.reshape(-1, feature.shape[-1])
    result = jnp.dot(flattened, weight, preferred_element_type=jnp.float32) + bias_row
    return result.reshape(feature.shape[:-1] + (weight.shape[1],))

def conv_three(widened, weight):
    padded = jnp.pad(widened, ((0, 0), (0, 0), (1, 1), (0, 0)))
    strip_rows = widened.shape[1] - 2
    width_cells = widened.shape[2]
    channels = widened.shape[3]
    result = jnp.zeros((widened.shape[0] * strip_rows * width_cells, weight.shape[2]), jnp.float32)
    for tap_row in range(3):
        band_rows = padded[:, tap_row:tap_row + strip_rows]
        stacked = jnp.concatenate([band_rows[:, :, 0:width_cells], band_rows[:, :, 1:width_cells + 1], band_rows[:, :, 2:width_cells + 2]], 3)
        result = result + jnp.dot(stacked.reshape(-1, 3 * channels), weight[tap_row], preferred_element_type=jnp.float32)
    return result.reshape(widened.shape[0], strip_rows, width_cells, weight.shape[2])

def group_sums(conv_out):
    dims_all = conv_out.shape
    grouped = conv_out.reshape(dims_all[0], -1, GROUPS, dims_all[3] // GROUPS)
    return (lax.optimization_barrier(jnp.sum(grouped, axis=(1, 3))), lax.optimization_barrier(jnp.sum(grouped * grouped, axis=(1, 3))))

def normalize(conv_out, totals, squares, entries, gain_row, shift_row):
    mean_val = totals / entries
    variance = squares / entries - mean_val * mean_val
    scale_inv = lax.rsqrt(variance + epsilon)
    dims_all = conv_out.shape
    grouped = conv_out.reshape(dims_all[0], dims_all[1], dims_all[2], GROUPS, dims_all[3] // GROUPS)
    centred = (grouped - mean_val[:, None, None, :, None]) * scale_inv[:, None, None, :, None]
    return (centred.reshape(dims_all) * gain_row + shift_row).astype(jnp.bfloat16)

def reference(level_two, level_three, level_four, level_five, lateral_two, lateral_three, lateral_four, lateral_five, lateral_bias, smooth_weight, norm_gain, norm_shift):
    features = (level_two, level_three, level_four, level_five)
    weights = (lateral_two, lateral_three, lateral_four, lateral_five)
    laterals = [lateral(features[level_idx], weights[level_idx], lateral_bias[level_idx]) for level_idx in range(4)]
    merged_maps = [None, None, None, None]
    merged_maps[3] = laterals[3].astype(jnp.bfloat16)
    for level_idx in (2, 1, 0):
        coarse = merged_maps[level_idx + 1].astype(jnp.float32)
        widened = jnp.concatenate([coarse[:, :1], coarse, coarse[:, -1:]], 1)
        upsampled = refine(edge_columns(refine(widened, 1)), 2)
        merged_maps[level_idx] = (laterals[level_idx] + upsampled).astype(jnp.bfloat16)
    outputs = []
    for level_idx in range(4):
        widened = jnp.pad(merged_maps[level_idx], ((0, 0), (1, 1), (0, 0), (0, 0)))
        conv_out = conv_three(widened, smooth_weight[level_idx])
        totals, squares = group_sums(conv_out)
        entries = float(conv_out.shape[1] * conv_out.shape[2] * (conv_out.shape[3] // GROUPS))
        outputs.append(normalize(conv_out, totals, squares, entries, norm_gain[level_idx], norm_shift[level_idx]))
    return (outputs[0], outputs[1], outputs[2], outputs[3])
```

```python
import jax
import jax.numpy as jnp
from jax import lax
from jax.experimental import pallas as pl
from jax.experimental.pallas import tpu as pltpu
from jax.sharding import PartitionSpec as P

MESH = pl.DeviceIdType.MESH
F32 = jnp.float32
BF16 = jnp.bfloat16
EPSILON = 1e-05
CHANNELS = 256
GROUP = 8
IMAGES = 2
COLS = (256, 128, 64, 32)
STRIP = (8, 4, 2, 1)
DEPTH = (256, 512, 1024, 2048)


def interpolation(cols, coarse_rows, pieces, width):
    coarse = cols // 2
    lanes = lax.broadcasted_iota(jnp.int32, (cols, width), 1)
    fine = lax.broadcasted_iota(jnp.int32, (cols, width), 0)
    block = lax.div(lanes, coarse)
    column = lax.rem(lanes, coarse)
    near = lax.div(fine, 2)
    far = jnp.clip(near + 2 * lax.rem(fine, 2) - 1, 0, coarse - 1)
    taps = jnp.where(column == near, 0.75, 0.0) + jnp.where(column == far, 0.25, 0.0)
    result = []
    for pairs in pieces:
        weight = jnp.zeros((cols, width), F32)
        for row, value in pairs:
            weight = jnp.where(block == row, value, weight)
        result.append((taps * weight).astype(BF16))
    return result


def lane_groups(values):
    lane = lax.broadcasted_iota(jnp.int32, values.shape, 1)
    for step in (1, 2, 4):
        upper = lax.rem(lax.div(lane, step), 2) == 1
        values = values + jnp.where(
            upper, pltpu.roll(values, step, axis=1), pltpu.roll(values, 128 - step, axis=1)
        )
    return values


def encode(stats, slot):
    rows = [
        jnp.sum(stats[image, kind], axis=0, keepdims=True)
        for image in range(IMAGES)
        for kind in range(2)
    ]
    packed = jnp.concatenate([r[:, :128] for r in rows] + [r[:, 128:] for r in rows], 0)
    packed = lane_groups(packed)
    lane = lax.broadcasted_iota(jnp.int32, packed.shape, 1)
    which = lax.broadcasted_iota(jnp.int32, packed.shape, 0)
    packed = jnp.where(lax.rem(lane, 8) == lax.rem(which, 4) + slot, packed, 0.0)
    return jnp.concatenate(
        [
            jnp.sum(packed[0:4], axis=0, keepdims=True),
            jnp.sum(packed[4:8], axis=0, keepdims=True),
        ],
        0,
    )


def decode(totals, slot):
    spread = jnp.concatenate([totals[0:1]] * 4 + [totals[1:2]] * 4, 0)
    lane = lax.broadcasted_iota(jnp.int32, spread.shape, 1)
    which = lax.broadcasted_iota(jnp.int32, spread.shape, 0)
    spread = jnp.where(lax.rem(lane, 8) == lax.rem(which, 4) + slot, spread, 0.0)
    spread = lane_groups(spread)
    row = lambda q: jnp.concatenate([spread[q : q + 1], spread[q + 4 : q + 5]], 1)
    return [(row(2 * image), row(2 * image + 1)) for image in range(IMAGES)]


def kernel(strips, *refs):
    (f2, f3, f4, f5, w2, w3, w4, w5, bias, smooth, gain, shift) = refs[:12]
    outs = refs[12:16]
    (
        f2v, f3v, f4v, f5v, w2v, w3v, w4v, w5v, biasv, smv, gainv, shiftv,
        xc2, xc3, xc4, xc5,
        t2, t3, t4,
        lat3, lat4,
        e5, e4, e3,
        r5, r4, r3, r2,
        rb2, rb3, rb4, rb5,
        cv2, cv3, cv4, cv5,
        stats,
        sendA, sendB, recvA, recvB,
        in_sem, edge_send, edge_recv, all_send, all_recv,
    ) = refs[16:]
    batch = lax.axis_index("batch")
    me = lax.axis_index("rows")
    peers = strips - 1
    above = lax.rem(me + strips - 1, strips)
    below = lax.rem(me + 1, strips)

    pairs = (
        (f5, f5v), (w5, w5v), (bias, biasv), (f4, f4v), (w4, w4v), (f3, f3v), (w3, w3v),
        (f2, f2v), (w2, w2v), (smooth.at[0], smv.at[0]), (smooth.at[1], smv.at[1]),
        (smooth.at[2], smv.at[2]), (smooth.at[3], smv.at[3]), (gain, gainv), (shift, shiftv),
    )
    loads = [pltpu.make_async_copy(s, d, in_sem.at[i]) for i, (s, d) in enumerate(pairs)]
    for load in loads:
        load.start()
    (lf5, lw5, lb, lf4, lw4, lf3, lw3, lf2, lw2, ls2, ls3, ls4, ls5, lg, lsh) = loads

    barrier = pltpu.get_barrier_semaphore()

    @pl.loop(1, strips)
    def _(k):
        pl.semaphore_signal(
            barrier, inc=1, device_id=(batch, lax.rem(me + k, strips)), device_id_type=MESH
        )

    first = me == 0
    last = me == strips - 1
    keep_top = jnp.where(first, 0.0, 1.0)
    keep_bottom = jnp.where(last, 0.0, 1.0)
    top_far = jnp.where(first, 0.0, 0.25)
    top_near = jnp.where(first, 1.0, 0.75)
    bottom_far = jnp.where(last, 0.0, 0.25)
    bottom_near = jnp.where(last, 1.0, 0.75)

    blocks = interpolation(
        64, 3,
        (
            ((0, 0.75), (1, 0.25)),
            ((0, top_far), (1, top_near)),
            ((1, bottom_near), (2, bottom_far)),
            ((1, 0.25), (2, 0.75)),
        ),
        128,
    )
    for i, block in enumerate(blocks):
        t4[64 * i : 64 * i + 64, :] = block
    blocks = interpolation(
        128, 4,
        (
            ((0, top_far), (1, top_near)),
            ((1, 0.75), (2, 0.25)),
            ((1, 0.25), (2, 0.75)),
            ((2, bottom_near), (3, bottom_far)),
            ((0, 0.75), (1, 0.25)),
            ((2, 0.25), (3, 0.75)),
        ),
        256,
    )
    for i, block in enumerate(blocks):
        t3[128 * i : 128 * i + 128, :] = block
    blocks = interpolation(
        256, 2,
        (
            ((0, 0.75), (1, 0.25)),
            ((0, 0.25), (1, 0.75)),
            ((0, top_far), (1, top_near)),
            ((0, bottom_near), (1, bottom_far)),
        ),
        256,
    )
    for place, which in ((0, 0), (1, 1), (2, 0), (3, 2), (4, 3), (5, 1)):
        t2[256 * place : 256 * place + 256, :] = blocks[which]

    for rb, cols in ((rb2, 256), (rb3, 128), (rb4, 64), (rb5, 32)):
        for copy in range(rb.shape[0]):
            for half in range(2):
                rb[copy, half, 0:8, :] = jnp.zeros((8, 128), F32)
                rb[copy, half, cols + 8 : cols + 16, :] = jnp.zeros((8, 128), F32)
    stats[...] = jnp.zeros_like(stats)

    def put_row(rb, copy, target, values):
        cols = values.shape[0]
        for half in range(2):
            rb[copy, half, 8 : 8 + cols, :] = values[:, 128 * half : 128 * half + 128]
        for tap in range(3):
            for half in range(2):
                target[:, 256 * tap + 128 * half : 256 * tap + 128 * half + 128] = rb[
                    copy, half, 7 + tap : 7 + tap + cols, :
                ].astype(BF16)

    def dot(a, b):
        return jnp.dot(a, b, preferred_element_type=F32)

    def edge(level, side, source, target, peer):
        return pltpu.make_async_remote_copy(
            src_ref=source,
            dst_ref=target,
            send_sem=edge_send.at[level, side],
            recv_sem=edge_recv.at[level, side],
            device_id=(batch, peer),
            device_id_type=MESH,
        )

    edges5 = (edge(3, 0, e5, r5.at[1], above), edge(3, 1, e5, r5.at[0], below))
    edges4 = (edge(2, 0, e4.at[0], r4.at[1], above), edge(2, 1, e4.at[1], r4.at[0], below))
    edges3 = (edge(1, 0, e3.at[0], r3.at[1], above), edge(1, 1, e3.at[1], r3.at[0], below))
    edges2 = (
        edge(0, 0, f2v.at[:, 0], r2.at[1], above),
        edge(0, 1, f2v.at[:, 7], r2.at[0], below),
    )

    lf5.wait()
    lw5.wait()
    lb.wait()
    merged = dot(f5v[...].reshape(64, 2048), w5v[...]) + biasv[3:4, :]
    e5[...] = merged.reshape(2, 32, 256).astype(BF16)
    pl.semaphore_wait(barrier, peers)
    for image in range(IMAGES):
        put_row(rb5, image, xc5.at[image, 1], merged[32 * image : 32 * image + 32])
    for copy in edges5:
        copy.start()

    lf4.wait()
    lw4.wait()
    flat = dot(f4v[...].reshape(256, 1024), w4v[...]) + biasv[2:3, :]
    for image in range(IMAGES):
        for row in range(2):
            part = flat[(2 * image + row) * 64 : (2 * image + row) * 64 + 64]
            e4[row, image] = part.astype(BF16)
            lat4[image, row] = part
    for copy in edges4:
        copy.start()

    lf3.wait()
    lw3.wait()
    for image in range(IMAGES):
        flat = dot(f3v[image].reshape(512, 512), w3v[...]) + biasv[1:2, :]
        e3[0, image] = flat[0:128].astype(BF16)
        e3[1, image] = flat[384:512].astype(BF16)
        lat3[image] = flat
    for copy in edges3:
        copy.start()
    lf2.wait()
    for copy in edges2:
        copy.start()

    for copy in edges5:
        copy.wait_recv()
    for image in range(IMAGES):
        put_row(rb5, image, xc5.at[image, 0], r5[0, image].astype(F32) * keep_top)
        put_row(rb5, 2 + image, xc5.at[image, 2], r5[1, image].astype(F32) * keep_bottom)
    for copy in edges4:
        copy.wait_recv()
    for image in range(IMAGES):
        coarse = jnp.concatenate(
            [xc5[image, :, :, 256:512].reshape(96, 256), jnp.zeros((32, 256), BF16)], 0
        )
        up = dot(t4[...], coarse)
        put_row(rb4, 0, xc4.at[image, 0], (up[0:64] + r4[0, image].astype(F32)) * keep_top)
        put_row(rb4, 1, xc4.at[image, 1], up[64:128] + lat4[image, 0])
        put_row(rb4, 2, xc4.at[image, 2], up[128:192] + lat4[image, 1])
        put_row(rb4, 3, xc4.at[image, 3], (up[192:256] + r4[1, image].astype(F32)) * keep_bottom)

    for image in range(IMAGES):
        up = dot(t3[0:512, :], xc4[image, :, :, 256:512].reshape(256, 256)) + lat3[image]
        for row in range(4):
            put_row(rb3, row, xc3.at[image, 1 + row], up[128 * row : 128 * row + 128])

    lw2.wait()

    def pair(image, p, features, weights):
        left = jnp.concatenate([features, weights], 1)
        coarse = xc3[image, pl.ds(p + 1, 2), :, 256:512].reshape(256, 256)
        right = jnp.concatenate([w2v[...], coarse], 0)
        return dot(left, right) + biasv[0:1, :]

    @pl.loop(0, IMAGES)
    def _(image):
        for p in range(3):
            both = pair(
                image, p, f2v[image, 2 * p + 1 : 2 * p + 3].reshape(512, 256), t2[0:512, :]
            )
            put_row(rb2, 0, xc2.at[image, 2 * p + 2], both[0:256])
            put_row(rb2, 1, xc2.at[image, 2 * p + 3], both[256:512])

    def tally(level, image, values):
        tiles = values.reshape(values.shape[0] // 8, 8, 256)
        stats[level, image, 0] += jnp.sum(tiles, axis=0)
        stats[level, image, 1] += jnp.sum(tiles * tiles, axis=0)

    def conv(xc, level, image, row, rows):
        cols = COLS[level]
        total = None
        for tap in range(3):
            band = xc[image, pl.ds(row + tap, rows)].reshape(rows * cols, 768)
            term = dot(band, smv[level, tap])
            total = term if total is None else total + term
        return total

    ls2.wait()

    def conv_two(image, row):
        values = conv(xc2, 0, image, row, 2)
        cv2[image, pl.ds(row * 256, 512), :] = values
        tally(0, image, values)

    @pl.loop(0, IMAGES)
    def _(image):
        @pl.loop(1, 3)
        def _(j):
            conv_two(image, 2 * j)

    for copy in edges3:
        copy.wait_recv()
    for image in range(IMAGES):
        up = dot(t3[512:768, :], xc4[image, :, :, 256:512].reshape(256, 256))
        put_row(rb3, 0, xc3.at[image, 0], (up[0:128] + r3[0, image].astype(F32)) * keep_top)
        put_row(rb3, 1, xc3.at[image, 5], (up[128:256] + r3[1, image].astype(F32)) * keep_bottom)
    for copy in edges2:
        copy.wait_recv()

    @pl.loop(0, IMAGES)
    def _(image):
        both = pair(
            image, -1,
            jnp.concatenate([r2[0, image], f2v[image, 0]], 0), t2[512:1024, :],
        )
        put_row(rb2, 0, xc2.at[image, 0], both[0:256] * keep_top)
        put_row(rb2, 1, xc2.at[image, 1], both[256:512])
        both = pair(
            image, 3,
            jnp.concatenate([f2v[image, 7], r2[1, image]], 0), t2[1024:1536, :],
        )
        put_row(rb2, 2, xc2.at[image, 8], both[0:256])
        put_row(rb2, 3, xc2.at[image, 9], both[256:512] * keep_bottom)

    @pl.loop(0, IMAGES)
    def _(image):
        @pl.loop(0, 2)
        def _(j):
            conv_two(image, 6 * j)

    def everyone(source, target, which):
        def copy_to(k):
            return pltpu.make_async_remote_copy(
                src_ref=source,
                dst_ref=target.at[k],
                send_sem=all_send.at[which, k],
                recv_sem=all_recv.at[which, k],
                device_id=(batch, lax.rem(me + 1 + k, strips)),
                device_id_type=MESH,
            )

        return copy_to

    sendA[...] = encode(stats.at[0], 0)
    copyA = everyone(sendA, recvA, 0)
    pl.loop(0, peers)(lambda k: copyA(k).start())

    ls3.wait()
    ls4.wait()
    ls5.wait()
    values = None
    for tap in range(3):
        term = dot(xc5[:, tap].reshape(64, 768), smv[3, tap])
        values = term if values is None else values + term
    cv5[...] = values
    for image in range(IMAGES):
        tally(3, image, values[32 * image : 32 * image + 32])
    values = None
    for tap in range(3):
        term = dot(xc4[:, tap : tap + 2].reshape(256, 768), smv[2, tap])
        values = term if values is None else values + term
    cv4[...] = values
    for image in range(IMAGES):
        tally(2, image, values[128 * image : 128 * image + 128])

    @pl.loop(0, IMAGES)
    def _(image):
        values = conv(xc3, 1, image, 0, 4)
        cv3[image] = values
        tally(1, image, values)

    sendB[...] = jnp.concatenate([encode(stats.at[1], 0) + encode(stats.at[2], 4),
                                  encode(stats.at[3], 0)], 0)
    copyB = everyone(sendB, recvB, 1)
    pl.loop(0, peers)(lambda k: copyB(k).start())

    def affine(level, sums, squares):
        entries = float(COLS[level] * strips * STRIP[level] * GROUP)
        mean = sums / entries
        variance = squares / entries - mean * mean
        scale = lax.rsqrt(variance + EPSILON) * gainv[level : level + 1, :]
        return mean, scale, shiftv[level : level + 1, :]

    def normalized(values, terms):
        mean, scale, offset = terms
        return ((values - mean) * scale + offset).astype(BF16)

    lg.wait()
    lsh.wait()
    pl.loop(0, peers)(lambda k: copyA(k).wait_recv())
    totals = sendA[...] + jnp.sum(recvA[...], axis=0)
    for image, (sums, squares) in enumerate(decode(totals, 0)):
        terms = affine(0, sums, squares)

        @pl.loop(0, 8)
        def _(row):
            outs[0][image, row] = normalized(cv2[image, pl.ds(row * 256, 256), :], terms)

    pl.loop(0, peers)(lambda k: copyB(k).wait_recv())
    totals = sendB[...] + jnp.sum(recvB[...], axis=0)
    for level, half, slot in ((1, 0, 0), (2, 0, 4), (3, 2, 0)):
        for image, (sums, squares) in enumerate(decode(totals[half : half + 2], slot)):
            terms = affine(level, sums, squares)
            if level == 1:
                values = cv3[image]
            elif level == 2:
                values = cv4[128 * image : 128 * image + 128]
            else:
                values = cv5[32 * image : 32 * image + 32]
            outs[level][image] = normalized(values, terms).reshape(
                STRIP[level], COLS[level], 256
            )

    for copies in (edges5, edges4, edges3, edges2):
        for copy in copies:
            copy.wait_send()
    pl.loop(0, peers)(lambda k: copyA(k).wait_send())
    pl.loop(0, peers)(lambda k: copyB(k).wait_send())


def solution(mesh):
    strips = mesh.shape["rows"]

    def per_device(*args):
        vmem = pltpu.VMEM
        scratch = [
            vmem((2, 8, 256, 256), BF16), vmem((2, 4, 128, 512), BF16),
            vmem((2, 2, 64, 1024), BF16), vmem((2, 1, 32, 2048), BF16),
            vmem((256, 256), BF16), vmem((512, 256), BF16),
            vmem((1024, 256), BF16), vmem((2048, 256), BF16),
            vmem((4, 256), F32), vmem((4, 3, 768, 256), BF16),
            vmem((4, 256), F32), vmem((4, 256), F32),
            vmem((2, 10, 256, 768), BF16), vmem((2, 6, 128, 768), BF16),
            vmem((2, 4, 64, 768), BF16), vmem((2, 3, 32, 768), BF16),
            vmem((1536, 256), BF16), vmem((768, 256), BF16), vmem((256, 128), BF16),
            vmem((2, 512, 256), F32), vmem((2, 2, 64, 256), F32),
            vmem((2, 32, 256), BF16), vmem((2, 2, 64, 256), BF16), vmem((2, 2, 128, 256), BF16),
            vmem((2, 2, 32, 256), BF16), vmem((2, 2, 64, 256), BF16),
            vmem((2, 2, 128, 256), BF16), vmem((2, 2, 256, 256), BF16),
            vmem((4, 2, 272, 128), F32), vmem((4, 2, 144, 128), F32),
            vmem((4, 2, 80, 128), F32), vmem((4, 2, 48, 128), F32),
            vmem((2, 2048, 256), F32), vmem((2, 512, 256), F32),
            vmem((256, 256), F32), vmem((64, 256), F32),
            vmem((4, 2, 2, 8, 256), F32),
            vmem((2, 128), F32), vmem((4, 128), F32),
            vmem((strips - 1, 2, 128), F32), vmem((strips - 1, 4, 128), F32),
            pltpu.SemaphoreType.DMA((15,)),
            pltpu.SemaphoreType.DMA((4, 2)), pltpu.SemaphoreType.DMA((4, 2)),
            pltpu.SemaphoreType.DMA((2, strips - 1)), pltpu.SemaphoreType.DMA((2, strips - 1)),
        ]
        results = pl.pallas_call(
            lambda *refs: kernel(strips, *refs),
            name="pyramid",
            out_shape=[
                pltpu.VMEM((IMAGES, STRIP[k], COLS[k], CHANNELS), BF16) for k in range(4)
            ],
            in_specs=[pl.BlockSpec(memory_space=pltpu.HBM)] * 12,
            out_specs=[pl.BlockSpec(memory_space=pltpu.VMEM)] * 4,
            scratch_shapes=scratch,
            compiler_params=pltpu.CompilerParams(
                collective_id=0, has_side_effects=True, vmem_limit_bytes=48 << 20
            ),
            cost_estimate=pl.CostEstimate(
                flops=7_430_000_000, bytes_accessed=13_300_000, transcendentals=0
            ),
        )(*(pltpu.with_memory_space_constraint(a, pltpu.HBM) for a in args))
        return tuple(results)

    rows = P("batch", "rows", None, None)
    return jax.shard_map(
        per_device,
        mesh=mesh,
        in_specs=(rows,) * 4 + (P(),) * 8,
        out_specs=(rows,) * 4,
        check_vma=False,
    )
```

```python
import jax
import jax.numpy as jnp
from jax import lax
from jax.experimental import pallas as pl
from jax.experimental.pallas import tpu as pltpu
from jax.sharding import PartitionSpec as P

MESH = pl.DeviceIdType.MESH
F32 = jnp.float32
BF16 = jnp.bfloat16
EPSILON = 1e-05
CHANNELS = 256
GROUP = 8
IMAGES = 2
COLS = (256, 128, 64, 32)
STRIP = (8, 4, 2, 1)
DEPTH = (256, 512, 1024, 2048)


def interpolation(cols, coarse_rows, pieces, width):
    coarse = cols // 2
    lanes = lax.broadcasted_iota(jnp.int32, (cols, width), 1)
    fine = lax.broadcasted_iota(jnp.int32, (cols, width), 0)
    block = lax.div(lanes, coarse)
    column = lax.rem(lanes, coarse)
    near = lax.div(fine, 2)
    far = jnp.clip(near + 2 * lax.rem(fine, 2) - 1, 0, coarse - 1)
    taps = jnp.where(column == near, 0.75, 0.0) + jnp.where(column == far, 0.25, 0.0)
    result = []
    for pairs in pieces:
        weight = jnp.zeros((cols, width), F32)
        for row, value in pairs:
            weight = jnp.where(block == row, value, weight)
        result.append((taps * weight).astype(BF16))
    return result


def lane_groups(values):
    lane = lax.broadcasted_iota(jnp.int32, values.shape, 1)
    for step in (1, 2, 4):
        upper = lax.rem(lax.div(lane, step), 2) == 1
        values = values + jnp.where(
            upper, pltpu.roll(values, step, axis=1), pltpu.roll(values, 128 - step, axis=1)
        )
    return values


def encode(stats):
    rows = [
        jnp.sum(stats[image, kind], axis=0, keepdims=True)
        for image in range(IMAGES)
        for kind in range(2)
    ]
    packed = jnp.concatenate([r[:, :128] for r in rows] + [r[:, 128:] for r in rows], 0)
    packed = lane_groups(packed)
    lane = lax.broadcasted_iota(jnp.int32, packed.shape, 1)
    which = lax.broadcasted_iota(jnp.int32, packed.shape, 0)
    return jnp.sum(jnp.where(lax.rem(lane, 8) == which, packed, 0.0), axis=0, keepdims=True)


def decode(totals):
    spread = jnp.broadcast_to(totals, (8, 128))
    lane = lax.broadcasted_iota(jnp.int32, spread.shape, 1)
    which = lax.broadcasted_iota(jnp.int32, spread.shape, 0)
    spread = lane_groups(jnp.where(lax.rem(lane, 8) == which, spread, 0.0))
    row = lambda q: jnp.concatenate([spread[q : q + 1], spread[q + 4 : q + 5]], 1)
    return [(row(2 * image), row(2 * image + 1)) for image in range(IMAGES)]


def kernel(strips, *refs):
    (f2, f3, f4, f5, w2, w3, w4, w5, bias, smooth, gain, shift) = refs[:12]
    outs = refs[12:16]
    (
        f2v, f3v, f4v, f5v, w2v, w3v, w4v, w5v, biasv, smv, gainv, shiftv,
        xc2, xc3, xc4, xc5,
        t2, t3, t4,
        lat3, lat4,
        e5, e4, e3,
        r5, r4, r3, r2,
        rb2, rb3, rb4, rb5,
        cv2, cv3, cv4, cv5,
        stats,
        sendA, sendB, recvA, recvB,
        in_sem, edge_send, edge_recv, all_send, all_recv,
    ) = refs[16:]
    current = []

    def phase(name):
        if current:
            current.pop().__exit__(None, None, None)
        if name:
            current.append(jax.named_scope(name))
            current[0].__enter__()

    phase("start")
    batch = lax.axis_index("batch")
    me = lax.axis_index("rows")
    peers = strips - 1
    above = lax.rem(me + strips - 1, strips)
    below = lax.rem(me + 1, strips)

    barrier = pltpu.get_barrier_semaphore()
    for k in [1, strips - 1] + list(range(2, strips - 1)):
        pl.semaphore_signal(
            barrier, inc=1, device_id=(batch, lax.rem(me + k, strips)), device_id_type=MESH
        )

    pairs = (
        (f5, f5v), (w5, w5v), (bias, biasv), (f4, f4v), (w4, w4v), (f3, f3v), (w3, w3v),
        (f2, f2v), (w2, w2v), (smooth.at[0], smv.at[0]), (smooth.at[1], smv.at[1]),
        (smooth.at[2], smv.at[2]), (smooth.at[3], smv.at[3]), (gain, gainv), (shift, shiftv),
    )
    loads = [pltpu.make_async_copy(s, d, in_sem.at[i]) for i, (s, d) in enumerate(pairs)]
    for load in loads:
        load.start()
    (lf5, lw5, lb, lf4, lw4, lf3, lw3, lf2, lw2, ls2, ls3, ls4, ls5, lg, lsh) = loads

    first = me == 0
    last = me == strips - 1
    keep_top = jnp.where(first, 0.0, 1.0)
    keep_bottom = jnp.where(last, 0.0, 1.0)
    top_far = jnp.where(first, 0.0, 0.25)
    top_near = jnp.where(first, 1.0, 0.75)
    bottom_far = jnp.where(last, 0.0, 0.25)
    bottom_near = jnp.where(last, 1.0, 0.75)

    phase("matrices")
    blocks = interpolation(
        64, 3,
        (
            ((0, 0.75), (1, 0.25)),
            ((0, top_far), (1, top_near)),
            ((1, bottom_near), (2, bottom_far)),
            ((1, 0.25), (2, 0.75)),
        ),
        128,
    )
    for i, block in enumerate(blocks):
        t4[64 * i : 64 * i + 64, :] = block
    blocks = interpolation(
        128, 4,
        (
            ((0, top_far), (1, top_near)),
            ((1, 0.75), (2, 0.25)),
            ((1, 0.25), (2, 0.75)),
            ((2, bottom_near), (3, bottom_far)),
            ((0, 0.75), (1, 0.25)),
            ((2, 0.25), (3, 0.75)),
        ),
        256,
    )
    for i, block in enumerate(blocks):
        t3[128 * i : 128 * i + 128, :] = block
    blocks = interpolation(
        256, 2,
        (
            ((0, 0.75), (1, 0.25)),
            ((0, 0.25), (1, 0.75)),
            ((0, top_far), (1, top_near)),
            ((0, bottom_near), (1, bottom_far)),
        ),
        256,
    )
    for place, which in ((0, 0), (1, 1), (2, 0), (3, 2), (4, 3), (5, 1)):
        t2[256 * place : 256 * place + 256, :] = blocks[which]

    for rb, cols in ((rb2, 256), (rb3, 128), (rb4, 64), (rb5, 32)):
        for copy in range(rb.shape[0]):
            for half in range(2):
                rb[copy, half, 0:8, :] = jnp.zeros((8, 128), F32)
                rb[copy, half, cols + 8 : cols + 16, :] = jnp.zeros((8, 128), F32)
    stats[...] = jnp.zeros_like(stats)

    def put_row(rb, copy, target, values):
        cols = values.shape[0]
        for half in range(2):
            rb[copy, half, 8 : 8 + cols, :] = values[:, 128 * half : 128 * half + 128]
        for tap in range(3):
            for half in range(2):
                target[2 * tap + half] = rb[copy, half, 7 + tap : 7 + tap + cols, :].astype(BF16)

    def middle(xc, image, row, rows):
        halves = [xc[image, row : row + rows, 2 + half] for half in range(2)]
        return jnp.concatenate([h.reshape(-1, 128) for h in halves], 1)

    def dot(a, b):
        return jnp.dot(a, b, preferred_element_type=F32)

    def edge(level, side, source, target, peer):
        return pltpu.make_async_remote_copy(
            src_ref=source,
            dst_ref=target,
            send_sem=edge_send.at[level, side],
            recv_sem=edge_recv.at[level, side],
            device_id=(batch, peer),
            device_id_type=MESH,
        )

    edges5 = (edge(3, 0, e5, r5.at[1], above), edge(3, 1, e5, r5.at[0], below))
    edges4 = (edge(2, 0, e4.at[0], r4.at[1], above), edge(2, 1, e4.at[1], r4.at[0], below))
    edges3 = (edge(1, 0, e3.at[0], r3.at[1], above), edge(1, 1, e3.at[1], r3.at[0], below))
    edges2 = (
        edge(0, 0, f2v.at[:, 0], r2.at[1], above),
        edge(0, 1, f2v.at[:, 7], r2.at[0], below),
    )

    phase("wait_load5")
    lf5.wait()
    lw5.wait()
    lb.wait()
    phase("lat5")
    merged = dot(f5v[...].reshape(64, 2048), w5v[...]) + biasv[3:4, :]
    e5[...] = merged.reshape(2, 32, 256).astype(BF16)
    phase("barrier")
    pl.semaphore_wait(barrier, peers)
    phase("put5")
    for image in range(IMAGES):
        put_row(rb5, image, xc5.at[image, 1], merged[32 * image : 32 * image + 32])
    for copy in edges5:
        copy.start()

    phase("wait_load4")
    lf4.wait()
    lw4.wait()
    phase("lat4")
    flat = dot(f4v[...].reshape(256, 1024), w4v[...]) + biasv[2:3, :]
    for image in range(IMAGES):
        for row in range(2):
            part = flat[(2 * image + row) * 64 : (2 * image + row) * 64 + 64]
            e4[row, image] = part.astype(BF16)
            lat4[image, row] = part
    for copy in edges4:
        copy.start()

    phase("wait_load3")
    lf3.wait()
    lw3.wait()
    phase("lat3")
    for image in range(IMAGES):
        flat = dot(f3v[image].reshape(512, 512), w3v[...]) + biasv[1:2, :]
        e3[0, image] = flat[0:128].astype(BF16)
        e3[1, image] = flat[384:512].astype(BF16)
        lat3[image] = flat
    for copy in edges3:
        copy.start()
    phase("wait_load2")
    lf2.wait()
    for copy in edges2:
        copy.start()

    phase("lat2")
    lw2.wait()

    @pl.loop(0, IMAGES)
    def _(image):
        for part in range(2):
            cv2[image, 1024 * part : 1024 * part + 1024, :] = (
                dot(f2v[image, 4 * part : 4 * part + 4].reshape(1024, 256), w2v[...])
                + biasv[0:1, :]
            )

    phase("wait_edge5")
    for copy in edges5:
        copy.wait_recv()
    phase("halo5")
    for image in range(IMAGES):
        put_row(rb5, image, xc5.at[image, 0], r5[0, image].astype(F32) * keep_top)
        put_row(rb5, 2 + image, xc5.at[image, 2], r5[1, image].astype(F32) * keep_bottom)
    phase("wait_edge4")
    for copy in edges4:
        copy.wait_recv()
    phase("merge4")
    for image in range(IMAGES):
        coarse = jnp.concatenate(
            [middle(xc5, image, 0, 3), jnp.zeros((32, 256), BF16)], 0
        )
        up = dot(t4[...], coarse)
        put_row(rb4, 0, xc4.at[image, 0], (up[0:64] + r4[0, image].astype(F32)) * keep_top)
        put_row(rb4, 1, xc4.at[image, 1], up[64:128] + lat4[image, 0])
        put_row(rb4, 2, xc4.at[image, 2], up[128:192] + lat4[image, 1])
        put_row(rb4, 3, xc4.at[image, 3], (up[192:256] + r4[1, image].astype(F32)) * keep_bottom)

    phase("merge3")
    for image in range(IMAGES):
        up = dot(t3[0:512, :], middle(xc4, image, 0, 4)) + lat3[image]
        for row in range(4):
            put_row(rb3, row, xc3.at[image, 1 + row], up[128 * row : 128 * row + 128])

    phase("wait_w2")

    def pair(image, p, weights):
        return dot(weights, middle(xc3, image, p + 1, 2))

    phase("merge2")
    @pl.loop(0, IMAGES)
    def _(image):
        for p in range(3):
            both = pair(image, p, t2[0:512, :])
            for row in range(2):
                start = 512 * p + 256 + 256 * row
                put_row(
                    rb2, row, xc2.at[image, 2 * p + 2 + row],
                    both[256 * row : 256 * row + 256] + cv2[image, start : start + 256, :],
                )

    def tally(level, image, values):
        tiles = values.reshape(values.shape[0] // 8, 8, 256)
        stats[level, image, 0] += jnp.sum(tiles, axis=0)
        stats[level, image, 1] += jnp.sum(tiles * tiles, axis=0)

    def product(bands, level):
        total = None
        for tap, slabs in enumerate(bands):
            term = dot(jnp.concatenate(slabs, 1), smv[level, tap])
            total = term if total is None else total + term
        return total

    def conv(xc, level, image, row, rows):
        return product(
            [
                [xc[image, row + tap : row + tap + rows, slab].reshape(-1, 128) for slab in range(6)]
                for tap in range(3)
            ],
            level,
        )

    phase("wait_s2")
    ls2.wait()

    def conv_two(image, row):
        values = conv(xc2, 0, image, row, 2)
        cv2[image, row * 256 : row * 256 + 512, :] = values
        tally(0, image, values)

    phase("conv2a")
    @pl.loop(0, IMAGES)
    def _(image):
        for row in (2, 4):
            conv_two(image, row)

    phase("wait_edge3")
    for copy in edges3:
        copy.wait_recv()
    phase("halo3")
    for image in range(IMAGES):
        up = dot(t3[512:768, :], middle(xc4, image, 0, 4))
        put_row(rb3, 0, xc3.at[image, 0], (up[0:128] + r3[0, image].astype(F32)) * keep_top)
        put_row(rb3, 1, xc3.at[image, 5], (up[128:256] + r3[1, image].astype(F32)) * keep_bottom)
    phase("wait_edge2")
    for copy in edges2:
        copy.wait_recv()

    phase("merge2b")
    @pl.loop(0, IMAGES)
    def _(image):
        both = pair(image, -1, t2[512:1024, :])
        outside = dot(r2[0, image], w2v[...]) + biasv[0:1, :]
        put_row(rb2, 0, xc2.at[image, 0], (both[0:256] + outside) * keep_top)
        put_row(rb2, 1, xc2.at[image, 1], both[256:512] + cv2[image, 0:256, :])
        both = pair(image, 3, t2[1024:1536, :])
        outside = dot(r2[1, image], w2v[...]) + biasv[0:1, :]
        put_row(rb2, 2, xc2.at[image, 8], both[0:256] + cv2[image, 1792:2048, :])
        put_row(rb2, 3, xc2.at[image, 9], (both[256:512] + outside) * keep_bottom)

    phase("conv2b")
    @pl.loop(0, IMAGES)
    def _(image):
        for row in (0, 6):
            conv_two(image, row)

    phase("conv54")
    ls4.wait()
    ls5.wait()
    values = product(
        [[xc5[:, tap, slab].reshape(64, 128) for slab in range(6)] for tap in range(3)], 3
    )
    cv5[...] = values
    for image in range(IMAGES):
        tally(3, image, values[32 * image : 32 * image + 32])
    values = product(
        [
            [xc4[:, tap : tap + 2, slab].reshape(256, 128) for slab in range(6)]
            for tap in range(3)
        ],
        2,
    )
    cv4[...] = values
    for image in range(IMAGES):
        tally(2, image, values[128 * image : 128 * image + 128])

    def everyone(source, target, which):
        return [
            pltpu.make_async_remote_copy(
                src_ref=source,
                dst_ref=target.at[k],
                send_sem=all_send.at[which],
                recv_sem=all_recv.at[which],
                device_id=(batch, lax.rem(me + 1 + k, strips)),
                device_id_type=MESH,
            )
            for k in range(peers)
        ]

    phase("encodeA")
    sendA[...] = jnp.concatenate(
        [encode(stats.at[0]), encode(stats.at[2]), encode(stats.at[3]), jnp.zeros((1, 128), F32)], 0
    )
    for copy in everyone(sendA, recvA, 0):
        copy.start()

    phase("conv3")
    ls3.wait()
    for image in range(IMAGES):
        values = conv(xc3, 1, image, 0, 4)
        cv3[image] = values
        tally(1, image, values)

    phase("encodeB")
    sendB[...] = encode(stats.at[1])
    for copy in everyone(sendB, recvB, 1):
        copy.start()

    def affine(level, sums, squares):
        entries = float(COLS[level] * strips * STRIP[level] * GROUP)
        mean = sums / entries
        variance = squares / entries - mean * mean
        scale = lax.rsqrt(variance + EPSILON) * gainv[level : level + 1, :]
        return mean, scale, shiftv[level : level + 1, :]

    def normalized(values, terms):
        mean, scale, offset = terms
        return ((values - mean) * scale + offset).astype(BF16)

    lg.wait()
    lsh.wait()
    def finish(level, totals):
        for image, (sums, squares) in enumerate(decode(totals)):
            terms = affine(level, sums, squares)
            if level == 0:

                @pl.loop(0, 8)
                def _(row):
                    outs[0][image, row] = normalized(cv2[image, pl.ds(row * 256, 256), :], terms)

                continue
            if level == 1:
                values = cv3[image]
            elif level == 2:
                values = cv4[128 * image : 128 * image + 128]
            else:
                values = cv5[32 * image : 32 * image + 32]
            outs[level][image] = normalized(values, terms).reshape(
                STRIP[level], COLS[level], 256
            )

    phase("wait_A")
    pltpu.make_async_copy(recvA, recvA, all_recv.at[0]).wait()
    phase("normA")
    totals = sendA[...] + jnp.sum(recvA[...], axis=0)
    finish(0, totals[0:1])
    finish(2, totals[1:2])
    finish(3, totals[2:3])

    phase("wait_sends")
    for copies in (edges5, edges4, edges3, edges2):
        for copy in copies:
            copy.wait_send()
    pltpu.make_async_copy(recvA, recvA, all_send.at[0]).wait()
    pltpu.make_async_copy(recvB, recvB, all_send.at[1]).wait()
    phase("wait_B")
    pltpu.make_async_copy(recvB, recvB, all_recv.at[1]).wait()
    phase("normB")
    totals = sendB[...] + jnp.sum(recvB[...], axis=0)
    finish(1, totals)
    phase(None)


def write_out(*refs):
    sems = refs[8]
    copies = [pltpu.make_async_copy(refs[k], refs[4 + k], sems.at[k]) for k in range(4)]
    for copy in copies:
        copy.start()
    for copy in copies:
        copy.wait()


def solution(mesh):
    strips = mesh.shape["rows"]

    def per_device(*args):
        vmem = pltpu.VMEM
        scratch = [
            vmem((2, 8, 256, 256), BF16), vmem((2, 4, 128, 512), BF16),
            vmem((2, 2, 64, 1024), BF16), vmem((2, 1, 32, 2048), BF16),
            vmem((256, 256), BF16), vmem((512, 256), BF16),
            vmem((1024, 256), BF16), vmem((2048, 256), BF16),
            vmem((4, 256), F32), vmem((4, 3, 768, 256), BF16),
            vmem((4, 256), F32), vmem((4, 256), F32),
            vmem((2, 10, 6, 256, 128), BF16), vmem((2, 6, 6, 128, 128), BF16),
            vmem((2, 4, 6, 64, 128), BF16), vmem((2, 3, 6, 32, 128), BF16),
            vmem((1536, 256), BF16), vmem((768, 256), BF16), vmem((256, 128), BF16),
            vmem((2, 512, 256), F32), vmem((2, 2, 64, 256), F32),
            vmem((2, 32, 256), BF16), vmem((2, 2, 64, 256), BF16), vmem((2, 2, 128, 256), BF16),
            vmem((2, 2, 32, 256), BF16), vmem((2, 2, 64, 256), BF16),
            vmem((2, 2, 128, 256), BF16), vmem((2, 2, 256, 256), BF16),
            vmem((4, 2, 272, 128), F32), vmem((4, 2, 144, 128), F32),
            vmem((4, 2, 80, 128), F32), vmem((4, 2, 48, 128), F32),
            vmem((2, 2048, 256), F32), vmem((2, 512, 256), F32),
            vmem((256, 256), F32), vmem((64, 256), F32),
            vmem((4, 2, 2, 8, 256), F32),
            vmem((4, 128), F32), vmem((1, 128), F32),
            vmem((strips - 1, 4, 128), F32), vmem((strips - 1, 1, 128), F32),
            pltpu.SemaphoreType.DMA((15,)),
            pltpu.SemaphoreType.DMA((4, 2)), pltpu.SemaphoreType.DMA((4, 2)),
            pltpu.SemaphoreType.DMA((2,)), pltpu.SemaphoreType.DMA((2,)),
        ]
        results = pl.pallas_call(
            lambda *refs: kernel(strips, *refs),
            name="pyramid",
            out_shape=[
                pltpu.VMEM((IMAGES, STRIP[k], COLS[k], CHANNELS), BF16) for k in range(4)
            ],
            in_specs=[pl.BlockSpec(memory_space=pltpu.HBM)] * 12,
            out_specs=[pl.BlockSpec(memory_space=pltpu.VMEM)] * 4,
            scratch_shapes=scratch,
            compiler_params=pltpu.CompilerParams(
                collective_id=0, has_side_effects=True, vmem_limit_bytes=48 << 20
            ),
            cost_estimate=pl.CostEstimate(
                flops=7_430_000_000, bytes_accessed=13_300_000, transcendentals=0
            ),
        )(*(pltpu.with_memory_space_constraint(a, pltpu.HBM) for a in args))
        return tuple(
            pl.pallas_call(
                write_out,
                name="write",
                out_shape=[jax.ShapeDtypeStruct(r.shape, r.dtype) for r in results],
                in_specs=[pl.BlockSpec(memory_space=pltpu.VMEM)] * 4,
                out_specs=[pl.BlockSpec(memory_space=pltpu.HBM)] * 4,
                scratch_shapes=[pltpu.SemaphoreType.DMA((4,))],
                cost_estimate=pl.CostEstimate(
                    flops=0, bytes_accessed=5_600_000, transcendentals=0
                ),
            )(*(pltpu.with_memory_space_constraint(r, pltpu.VMEM) for r in results))
        )

    rows = P("batch", "rows", None, None)
    return jax.shard_map(
        per_device,
        mesh=mesh,
        in_specs=(rows,) * 4 + (P(),) * 8,
        out_specs=(rows,) * 4,
        check_vma=False,
    )
```

```python
import jax
import jax.numpy as jnp
from jax import lax
from jax.experimental import pallas as pl
from jax.experimental.pallas import tpu as pltpu
from jax.sharding import PartitionSpec as P

MESH = pl.DeviceIdType.MESH
F32 = jnp.float32
BF16 = jnp.bfloat16
EPSILON = 1e-05
CHANNELS = 256
GROUP = 8
IMAGES = 2
COLS = (256, 128, 64, 32)
STRIP = (8, 4, 2, 1)
DEPTH = (256, 512, 1024, 2048)
SIDE = 4


def interpolation(cols, coarse_rows, pieces, width):
    coarse = cols // 2
    lanes = lax.broadcasted_iota(jnp.int32, (cols, width), 1)
    fine = lax.broadcasted_iota(jnp.int32, (cols, width), 0)
    block = lax.div(lanes, coarse)
    column = lax.rem(lanes, coarse)
    near = lax.div(fine, 2)
    far = jnp.clip(near + 2 * lax.rem(fine, 2) - 1, 0, coarse - 1)
    taps = jnp.where(column == near, 0.75, 0.0) + jnp.where(column == far, 0.25, 0.0)
    result = []
    for pairs in pieces:
        weight = jnp.zeros((cols, width), F32)
        for row, value in pairs:
            weight = jnp.where(block == row, value, weight)
        result.append((taps * weight).astype(BF16))
    return result


def lane_groups(values):
    lane = lax.broadcasted_iota(jnp.int32, values.shape, 1)
    for step in (1, 2, 4):
        upper = lax.rem(lax.div(lane, step), 2) == 1
        values = values + jnp.where(
            upper, pltpu.roll(values, step, axis=1), pltpu.roll(values, 128 - step, axis=1)
        )
    return values


def encode(stats):
    rows = [
        jnp.sum(stats[image, kind], axis=0, keepdims=True)
        for image in range(IMAGES)
        for kind in range(2)
    ]
    packed = jnp.concatenate([r[:, :128] for r in rows] + [r[:, 128:] for r in rows], 0)
    packed = lane_groups(packed)
    lane = lax.broadcasted_iota(jnp.int32, packed.shape, 1)
    which = lax.broadcasted_iota(jnp.int32, packed.shape, 0)
    return jnp.sum(jnp.where(lax.rem(lane, 8) == which, packed, 0.0), axis=0, keepdims=True)


def decode(totals):
    spread = jnp.broadcast_to(totals, (8, 128))
    lane = lax.broadcasted_iota(jnp.int32, spread.shape, 1)
    which = lax.broadcasted_iota(jnp.int32, spread.shape, 0)
    spread = lane_groups(jnp.where(lax.rem(lane, 8) == which, spread, 0.0))
    row = lambda q: jnp.concatenate([spread[q : q + 1], spread[q + 4 : q + 5]], 1)
    return [(row(2 * image), row(2 * image + 1)) for image in range(IMAGES)]


def affine_of(level, strips, totals, gain, offset):
    entries = float(COLS[level] * strips * STRIP[level] * GROUP)
    result = []
    for sums, squares in decode(totals):
        mean = sums / entries
        variance = squares / entries - mean * mean
        result.append((mean, lax.rsqrt(variance + EPSILON) * gain, offset))
    return result


def normalized(values, terms):
    mean, scale, offset = terms
    return ((values - mean) * scale + offset).astype(BF16)


def kernel(strips, *refs):
    (f2, f3, f4, f5, w2, w3, w4, w5, bias, smooth, gain, shift) = refs[:12]
    outs = {0: refs[12], 2: refs[13], 3: refs[14], 4: refs[16]}
    cv3 = refs[15]
    norms = refs[17]
    (
        f2v, f3v, f4v, f5v, w2v, w3v, w4v, w5v, biasv, smv, gainv, shiftv,
        xc2, xc3, xc4, xc5,
        t2, t3, t4,
        lat3, lat4,
        e5, e4, e3,
        r5, r4, r3, r2,
        rb2, rb3, rb4, rb5,
        cv2, cv4, cv5,
        stats,
        sendA, sendB, recvA, recvB,
        in_sem, edge_send, edge_recv, all_send, all_recv, entered,
    ) = refs[18:]
    current = []

    def phase(name):
        if current:
            current.pop().__exit__(None, None, None)
        if name:
            current.append(jax.named_scope(name))
            current[0].__enter__()

    phase("start")
    batch = lax.axis_index("batch")
    me = lax.axis_index("rows")
    peers = strips - 1
    above = lax.rem(me + strips - 1, strips)
    below = lax.rem(me + 1, strips)

    pairs = (
        (f5, f5v), (w5, w5v), (bias, biasv), (f4, f4v), (w4, w4v), (f3, f3v), (w3, w3v),
        (f2, f2v), (w2, w2v), (smooth.at[0], smv.at[0]), (smooth.at[1], smv.at[1]),
        (smooth.at[2], smv.at[2]), (smooth.at[3], smv.at[3]), (gain, gainv), (shift, shiftv),
    )
    loads = [pltpu.make_async_copy(s, d, in_sem.at[i]) for i, (s, d) in enumerate(pairs)]
    for load in loads:
        load.start()
    (lf5, lw5, lb, lf4, lw4, lf3, lw3, lf2, lw2, ls2, ls3, ls4, ls5, lg, lsh) = loads

    barrier = pltpu.get_barrier_semaphore()
    core = lax.rem(me, 2)
    x = lax.rem(lax.div(me, 2), SIDE)
    y = lax.div(me, 2 * SIDE)
    line = [
        (y * SIDE + lax.rem(x + i, SIDE)) * 2 + lax.rem(core + c, 2)
        for i in (0, 1, SIDE - 1, *range(2, SIDE - 1))
        for c in range(2)
        if i or c
    ]
    column = [(lax.rem(y + i, SIDE) * SIDE + x) * 2 + core for i in range(1, SIDE)]
    ends_line = jnp.logical_and(lax.rem(me, 2 * SIDE) == 2 * SIDE - 1, me < strips - 1)
    opens_line = jnp.logical_and(lax.rem(me, 2 * SIDE) == 0, me > 0)
    has_above = me > 0
    has_below = me < strips - 1

    def greet(semaphore, peer):
        pl.semaphore_signal(semaphore, inc=1, device_id=(batch, peer), device_id_type=MESH)

    pl.when(ends_line)(lambda: greet(barrier, below))
    pl.when(opens_line)(lambda: greet(barrier, above))
    for peer in line + column:
        greet(barrier, peer)

    first = me == 0
    last = me == strips - 1
    keep_top = jnp.where(first, 0.0, 1.0)
    keep_bottom = jnp.where(last, 0.0, 1.0)
    top_far = jnp.where(first, 0.0, 0.25)
    top_near = jnp.where(first, 1.0, 0.75)
    bottom_far = jnp.where(last, 0.0, 0.25)
    bottom_near = jnp.where(last, 1.0, 0.75)

    phase("matrices")
    blocks = interpolation(
        64, 3,
        (
            ((0, 0.75), (1, 0.25)),
            ((0, top_far), (1, top_near)),
            ((1, bottom_near), (2, bottom_far)),
            ((1, 0.25), (2, 0.75)),
        ),
        128,
    )
    for i, block in enumerate(blocks):
        t4[64 * i : 64 * i + 64, :] = block
    blocks = interpolation(
        128, 4,
        (
            ((0, top_far), (1, top_near)),
            ((1, 0.75), (2, 0.25)),
            ((1, 0.25), (2, 0.75)),
            ((2, bottom_near), (3, bottom_far)),
            ((0, 0.75), (1, 0.25)),
            ((2, 0.25), (3, 0.75)),
        ),
        256,
    )
    for i, block in enumerate(blocks):
        t3[128 * i : 128 * i + 128, :] = block
    blocks = interpolation(
        256, 2,
        (
            ((0, 0.75), (1, 0.25)),
            ((0, 0.25), (1, 0.75)),
            ((0, top_far), (1, top_near)),
            ((0, bottom_near), (1, bottom_far)),
        ),
        256,
    )
    for place, which in ((0, 0), (1, 1), (2, 0), (3, 2), (4, 3), (5, 1)):
        t2[256 * place : 256 * place + 256, :] = blocks[which]

    for rb, cols in ((rb2, 256), (rb3, 128), (rb4, 64), (rb5, 32)):
        for copy in range(rb.shape[0]):
            for half in range(2):
                rb[copy, half, 0:8, :] = jnp.zeros((8, 128), F32)
                rb[copy, half, cols + 8 : cols + 16, :] = jnp.zeros((8, 128), F32)
    stats[...] = jnp.zeros_like(stats)

    def put_row(rb, copy, target, values):
        cols = values.shape[0]
        for half in range(2):
            rb[copy, half, 8 : 8 + cols, :] = values[:, 128 * half : 128 * half + 128]
        for half in range(2):
            target[2 + half] = values[:, 128 * half : 128 * half + 128].astype(BF16)
            for tap in (0, 2):
                target[2 * tap + half] = rb[copy, half, 7 + tap : 7 + tap + cols, :].astype(BF16)

    def middle(xc, image, row, rows):
        halves = [xc[image, row : row + rows, 2 + half] for half in range(2)]
        return jnp.concatenate([h.reshape(-1, 128) for h in halves], 1)

    def dot(a, b):
        return jnp.dot(a, b, preferred_element_type=F32)

    def edge(level, side, source, target, peer):
        return pltpu.make_async_remote_copy(
            src_ref=source,
            dst_ref=target,
            send_sem=edge_send.at[level, side],
            recv_sem=edge_recv.at[level, side],
            device_id=(batch, peer),
            device_id_type=MESH,
        )

    edges5 = (edge(3, 0, e5, r5.at[1], above), edge(3, 1, e5, r5.at[0], below))
    edges4 = (edge(2, 0, e4.at[0], r4.at[1], above), edge(2, 1, e4.at[1], r4.at[0], below))
    edges3 = (edge(1, 0, e3.at[0], r3.at[1], above), edge(1, 1, e3.at[1], r3.at[0], below))
    edges2 = (
        edge(0, 0, f2v.at[:, 0], r2.at[1], above),
        edge(0, 1, f2v.at[:, 7], r2.at[0], below),
    )

    def send(*levels):
        @pl.when(has_above)
        def _():
            for pair_of in levels:
                pair_of[0].start()

        @pl.when(has_below)
        def _():
            for pair_of in levels:
                pair_of[1].start()

    def receive(*levels):
        @pl.when(has_below)
        def _():
            for pair_of in levels:
                pair_of[0].wait_recv()

        @pl.when(has_above)
        def _():
            for pair_of in levels:
                pair_of[1].wait_recv()

    for side, missing in ((0, first), (1, last)):

        @pl.when(missing)
        def _():
            for halo in (r5, r4, r3, r2):
                halo[side] = jnp.zeros_like(halo[side])

    phase("wait_load54")
    lf5.wait()
    lw5.wait()
    lb.wait()
    lf4.wait()
    lw4.wait()
    phase("lat54")
    merged = dot(f5v[...].reshape(64, 2048), w5v[...]) + biasv[3:4, :]
    e5[...] = merged.reshape(2, 32, 256).astype(BF16)
    flat = dot(f4v[...].reshape(256, 1024), w4v[...]) + biasv[2:3, :]
    for image in range(IMAGES):
        put_row(rb5, image, xc5.at[image, 1], merged[32 * image : 32 * image + 32])
        for row in range(2):
            part = flat[(2 * image + row) * 64 : (2 * image + row) * 64 + 64]
            e4[row, image] = part.astype(BF16)
            lat4[image, row] = part
    phase("barrier")
    pl.semaphore_wait(
        barrier,
        len(line + column) + jnp.where(jnp.logical_or(ends_line, opens_line), 1, 0),
    )
    send(edges5, edges4)
    for peer in column:
        greet(entered, peer)

    phase("wait_load3")
    lf3.wait()
    lw3.wait()
    phase("lat3")
    for image in range(IMAGES):
        flat = dot(f3v[image].reshape(512, 512), w3v[...]) + biasv[1:2, :]
        e3[0, image] = flat[0:128].astype(BF16)
        e3[1, image] = flat[384:512].astype(BF16)
        lat3[image] = flat
    send(edges3)
    phase("wait_load2")
    lf2.wait()
    send(edges2)

    phase("lat2")
    lw2.wait()

    @pl.loop(0, IMAGES)
    def _(image):
        for part in range(2):
            cv2[image, 1024 * part : 1024 * part + 1024, :] = (
                dot(f2v[image, 4 * part : 4 * part + 4].reshape(1024, 256), w2v[...])
                + biasv[0:1, :]
            )
    ls2.wait()

    phase("wait_edge5")
    receive(edges5, edges4)
    phase("merge")
    for image in range(IMAGES):
        put_row(rb5, 2 + image, xc5.at[image, 0], r5[0, image].astype(F32) * keep_top)
        put_row(rb5, 4 + image, xc5.at[image, 2], r5[1, image].astype(F32) * keep_bottom)
    for image in range(IMAGES):
        coarse = jnp.concatenate(
            [middle(xc5, image, 0, 3), jnp.zeros((32, 256), BF16)], 0
        )
        up = dot(t4[...], coarse)
        put_row(rb4, 4 * image + 0, xc4.at[image, 0], (up[0:64] + r4[0, image].astype(F32)) * keep_top)
        put_row(rb4, 4 * image + 1, xc4.at[image, 1], up[64:128] + lat4[image, 0])
        put_row(rb4, 4 * image + 2, xc4.at[image, 2], up[128:192] + lat4[image, 1])
        put_row(rb4, 4 * image + 3, xc4.at[image, 3], (up[192:256] + r4[1, image].astype(F32)) * keep_bottom)

    for image in range(IMAGES):
        up = dot(t3[0:512, :], middle(xc4, image, 0, 4)) + lat3[image]
        for row in range(4):
            put_row(rb3, 4 * image + row, xc3.at[image, 1 + row], up[128 * row : 128 * row + 128])

    def pair(image, p, weights):
        return dot(weights, middle(xc3, image, p + 1, 2))

    def merge_middle(image):
        for p in range(3):
            both = pair(image, p, t2[0:512, :])
            for row in range(2):
                start = 512 * p + 256 + 256 * row
                put_row(
                    rb2, 6 * image + 2 * p + row, xc2.at[image, 2 * p + 2 + row],
                    both[256 * row : 256 * row + 256] + cv2[image, start : start + 256, :],
                )

    def tally(level, image, values):
        tiles = values.reshape(values.shape[0] // 8, 8, 256)
        stats[level, image, 0] += jnp.sum(tiles, axis=0)
        stats[level, image, 1] += jnp.sum(tiles * tiles, axis=0)

    def product(bands, level):
        total = None
        for tap, slabs in enumerate(bands):
            term = dot(jnp.concatenate(slabs, 1), smv[level, tap])
            total = term if total is None else total + term
        return total

    def conv(xc, level, image, row, rows):
        return product(
            [
                [xc[image, row + tap : row + tap + rows, slab].reshape(-1, 128) for slab in range(6)]
                for tap in range(3)
            ],
            level,
        )

    def conv_two(image, row):
        values = conv(xc2, 0, image, row, 2)
        cv2[image, row * 256 : row * 256 + 512, :] = values
        tally(0, image, values)

    for image in range(IMAGES):
        merge_middle(image)
        for row in (2, 4):
            conv_two(image, row)

    phase("wait_edge3")
    receive(edges3, edges2)
    ls4.wait()
    ls5.wait()
    phase("rest2")
    for image in range(IMAGES):
        up = dot(t3[512:768, :], middle(xc4, image, 0, 4))
        put_row(rb3, 8 + image, xc3.at[image, 0], (up[0:128] + r3[0, image].astype(F32)) * keep_top)
        put_row(rb3, 10 + image, xc3.at[image, 5], (up[128:256] + r3[1, image].astype(F32)) * keep_bottom)
    def merge_ends(image):
        both = pair(image, -1, t2[512:1024, :])
        outside = dot(r2[0, image], w2v[...]) + biasv[0:1, :]
        base = 12 + 4 * image
        put_row(rb2, base, xc2.at[image, 0], (both[0:256] + outside) * keep_top)
        put_row(rb2, base + 1, xc2.at[image, 1], both[256:512] + cv2[image, 0:256, :])
        both = pair(image, 3, t2[1024:1536, :])
        outside = dot(r2[1, image], w2v[...]) + biasv[0:1, :]
        put_row(rb2, base + 2, xc2.at[image, 8], both[0:256] + cv2[image, 1792:2048, :])
        put_row(rb2, base + 3, xc2.at[image, 9], (both[256:512] + outside) * keep_bottom)

    for image in range(IMAGES):
        merge_ends(image)
        for row in (0, 6):
            conv_two(image, row)

    values = product(
        [[xc5[:, tap, slab].reshape(64, 128) for slab in range(6)] for tap in range(3)], 3
    )
    cv5[...] = values
    for image in range(IMAGES):
        tally(3, image, values[32 * image : 32 * image + 32])
    values = product(
        [
            [xc4[:, tap : tap + 2, slab].reshape(256, 128) for slab in range(6)]
            for tap in range(3)
        ],
        2,
    )
    cv4[...] = values
    for image in range(IMAGES):
        tally(2, image, values[128 * image : 128 * image + 128])

    def everyone(source, target, which):
        return [
            pltpu.make_async_remote_copy(
                src_ref=source,
                dst_ref=target.at[k],
                send_sem=all_send.at[which],
                recv_sem=all_recv.at[which],
                device_id=(batch, lax.rem(me + 1 + k, strips)),
                device_id_type=MESH,
            )
            for k in range(peers)
        ]

    phase("encodeA")
    sendA[...] = jnp.concatenate(
        [encode(stats.at[0]), encode(stats.at[2]), encode(stats.at[3]), jnp.zeros((1, 128), F32)], 0
    )
    pl.semaphore_wait(entered, len(column))
    for copy in everyone(sendA, recvA, 0):
        copy.start()

    phase("conv3")
    ls3.wait()
    for image in range(IMAGES):
        values = conv(xc3, 1, image, 0, 4)
        cv3[image] = values
        tally(1, image, values)

    phase("encodeB")
    sendB[...] = encode(stats.at[1])
    for copy in everyone(sendB, recvB, 1):
        copy.start()

    lg.wait()
    lsh.wait()
    norms[0:1, :] = gainv[1:2, :]
    norms[1:2, :] = shiftv[1:2, :]
    def finish(level, totals):
        affine = affine_of(level, strips, totals, gainv[level : level + 1], shiftv[level : level + 1])
        for image, terms in enumerate(affine):
            if level == 0:

                @pl.loop(0, 8)
                def _(row):
                    outs[0][image, row] = normalized(cv2[image, pl.ds(row * 256, 256), :], terms)

                continue
            if level == 2:
                values = cv4[128 * image : 128 * image + 128]
            else:
                values = cv5[32 * image : 32 * image + 32]
            outs[level][image] = normalized(values, terms).reshape(
                STRIP[level], COLS[level], 256
            )

    phase("wait_A")
    pltpu.make_async_copy(recvA, recvA, all_recv.at[0]).wait()
    phase("normA")
    totals = sendA[...] + jnp.sum(recvA[...], axis=0)
    finish(0, totals[0:1])
    finish(2, totals[1:2])
    finish(3, totals[2:3])

    phase("wait_sends")
    @pl.when(has_above)
    def _():
        for pair_of in (edges5, edges4, edges3, edges2):
            pair_of[0].wait_send()

    @pl.when(has_below)
    def _():
        for pair_of in (edges5, edges4, edges3, edges2):
            pair_of[1].wait_send()

    pltpu.make_async_copy(recvA, recvA, all_send.at[0]).wait()
    pltpu.make_async_copy(recvB, recvB, all_send.at[1]).wait()
    phase("wait_B")
    pltpu.make_async_copy(recvB, recvB, all_recv.at[1]).wait()
    phase("normB")
    outs[4][...] = sendB[...] + jnp.sum(recvB[...], axis=0)
    phase(None)


def write_out(strips, in2, in4, in5, values, totals, norms, out2, out3, out4, out5, made3, sems):
    copies = [
        pltpu.make_async_copy(source, target, sems.at[k])
        for k, (source, target) in enumerate(
            ((in2, out2), (in4, out4), (in5, out5), (made3, out3))
        )
    ]
    for copy in copies[:3]:
        copy.start()
    affine = affine_of(1, strips, totals[...], norms[0:1, :], norms[1:2, :])
    for image, terms in enumerate(affine):
        made3[image] = normalized(values[image], terms).reshape(STRIP[1], COLS[1], CHANNELS)
    copies[3].start()
    for copy in copies:
        copy.wait()


def solution(mesh):
    strips = mesh.shape["rows"]

    def per_device(*args):
        vmem = pltpu.VMEM
        scratch = [
            vmem((2, 8, 256, 256), BF16), vmem((2, 4, 128, 512), BF16),
            vmem((2, 2, 64, 1024), BF16), vmem((2, 1, 32, 2048), BF16),
            vmem((256, 256), BF16), vmem((512, 256), BF16),
            vmem((1024, 256), BF16), vmem((2048, 256), BF16),
            vmem((4, 256), F32), vmem((4, 3, 768, 256), BF16),
            vmem((4, 256), F32), vmem((4, 256), F32),
            vmem((2, 10, 6, 256, 128), BF16), vmem((2, 6, 6, 128, 128), BF16),
            vmem((2, 4, 6, 64, 128), BF16), vmem((2, 3, 6, 32, 128), BF16),
            vmem((1536, 256), BF16), vmem((768, 256), BF16), vmem((256, 128), BF16),
            vmem((2, 512, 256), F32), vmem((2, 2, 64, 256), F32),
            vmem((2, 32, 256), BF16), vmem((2, 2, 64, 256), BF16), vmem((2, 2, 128, 256), BF16),
            vmem((2, 2, 32, 256), BF16), vmem((2, 2, 64, 256), BF16),
            vmem((2, 2, 128, 256), BF16), vmem((2, 2, 256, 256), BF16),
            vmem((20, 2, 272, 128), F32), vmem((12, 2, 144, 128), F32),
            vmem((8, 2, 80, 128), F32), vmem((6, 2, 48, 128), F32),
            vmem((2, 2048, 256), F32), vmem((256, 256), F32), vmem((64, 256), F32),
            vmem((4, 2, 2, 8, 256), F32),
            vmem((4, 128), F32), vmem((1, 128), F32),
            vmem((strips - 1, 4, 128), F32), vmem((strips - 1, 1, 128), F32),
            pltpu.SemaphoreType.DMA((15,)),
            pltpu.SemaphoreType.DMA((4, 2)), pltpu.SemaphoreType.DMA((4, 2)),
            pltpu.SemaphoreType.DMA((2,)), pltpu.SemaphoreType.DMA((2,)),
            pltpu.SemaphoreType.REGULAR,
        ]
        results = pl.pallas_call(
            lambda *refs: kernel(strips, *refs),
            name="pyramid",
            out_shape=[
                pltpu.VMEM((IMAGES, STRIP[k], COLS[k], CHANNELS), BF16) for k in (0, 2, 3)
            ]
            + [
                pltpu.VMEM((IMAGES, STRIP[1] * COLS[1], CHANNELS), F32),
                pltpu.VMEM((1, 128), F32),
                pltpu.VMEM((2, CHANNELS), F32),
            ],
            in_specs=[pl.BlockSpec(memory_space=pltpu.HBM)] * 12,
            out_specs=[pl.BlockSpec(memory_space=pltpu.VMEM)] * 6,
            scratch_shapes=scratch,
            compiler_params=pltpu.CompilerParams(
                collective_id=0, has_side_effects=True, vmem_limit_bytes=48 << 20
            ),
            cost_estimate=pl.CostEstimate(
                flops=7_430_000_000, bytes_accessed=13_300_000, transcendentals=0
            ),
        )(*(pltpu.with_memory_space_constraint(a, pltpu.HBM) for a in args))
        return tuple(
            pl.pallas_call(
                lambda *refs: write_out(strips, *refs),
                name="write",
                out_shape=[
                    jax.ShapeDtypeStruct((IMAGES, STRIP[k], COLS[k], CHANNELS), BF16)
                    for k in range(4)
                ],
                in_specs=[pl.BlockSpec(memory_space=pltpu.VMEM)] * 6,
                out_specs=[pl.BlockSpec(memory_space=pltpu.HBM)] * 4,
                scratch_shapes=[
                    pltpu.VMEM((IMAGES, STRIP[1], COLS[1], CHANNELS), BF16),
                    pltpu.SemaphoreType.DMA((4,)),
                ],
                cost_estimate=pl.CostEstimate(
                    flops=0, bytes_accessed=5_600_000, transcendentals=0
                ),
            )(*(pltpu.with_memory_space_constraint(r, pltpu.VMEM) for r in results))
        )

    rows = P("batch", "rows", None, None)
    return jax.shard_map(
        per_device,
        mesh=mesh,
        in_specs=(rows,) * 4 + (P(),) * 8,
        out_specs=(rows,) * 4,
        check_vma=False,
    )
```

```python
import jax
import jax.numpy as jnp
from jax import lax
from jax.experimental import pallas as pl
from jax.experimental.pallas import tpu as pltpu
from jax.sharding import PartitionSpec as P

MESH = pl.DeviceIdType.MESH
F32 = jnp.float32
BF16 = jnp.bfloat16
EPSILON = 1e-05
CHANNELS = 256
GROUP = 8
IMAGES = 2
COLS = (256, 128, 64, 32)
STRIP = (8, 4, 2, 1)
DEPTH = (256, 512, 1024, 2048)
SIDE = 4


def interpolation(cols, coarse_rows, pieces, width):
    coarse = cols // 2
    lanes = lax.broadcasted_iota(jnp.int32, (cols, width), 1)
    fine = lax.broadcasted_iota(jnp.int32, (cols, width), 0)
    block = lax.div(lanes, coarse)
    column = lax.rem(lanes, coarse)
    near = lax.div(fine, 2)
    far = jnp.clip(near + 2 * lax.rem(fine, 2) - 1, 0, coarse - 1)
    taps = jnp.where(column == near, 0.75, 0.0) + jnp.where(column == far, 0.25, 0.0)
    result = []
    for pairs in pieces:
        weight = jnp.zeros((cols, width), F32)
        for row, value in pairs:
            weight = jnp.where(block == row, value, weight)
        result.append((taps * weight).astype(BF16))
    return result


def lane_groups(values):
    lane = lax.broadcasted_iota(jnp.int32, values.shape, 1)
    for step in (1, 2, 4):
        upper = lax.rem(lax.div(lane, step), 2) == 1
        values = values + jnp.where(
            upper, pltpu.roll(values, step, axis=1), pltpu.roll(values, 128 - step, axis=1)
        )
    return values


def encode(stats):
    rows = [
        jnp.sum(stats[image, kind], axis=0, keepdims=True)
        for image in range(IMAGES)
        for kind in range(2)
    ]
    packed = jnp.concatenate([r[:, :128] for r in rows] + [r[:, 128:] for r in rows], 0)
    packed = lane_groups(packed)
    lane = lax.broadcasted_iota(jnp.int32, packed.shape, 1)
    which = lax.broadcasted_iota(jnp.int32, packed.shape, 0)
    return jnp.sum(jnp.where(lax.rem(lane, 8) == which, packed, 0.0), axis=0, keepdims=True)


def decode(totals):
    spread = jnp.broadcast_to(totals, (8, 128))
    lane = lax.broadcasted_iota(jnp.int32, spread.shape, 1)
    which = lax.broadcasted_iota(jnp.int32, spread.shape, 0)
    spread = lane_groups(jnp.where(lax.rem(lane, 8) == which, spread, 0.0))
    row = lambda q: jnp.concatenate([spread[q : q + 1], spread[q + 4 : q + 5]], 1)
    return [(row(2 * image), row(2 * image + 1)) for image in range(IMAGES)]


def affine_of(level, strips, totals, gain, shift):
    entries = float(COLS[level] * strips * STRIP[level] * GROUP)
    result = []
    for sums, squares in decode(totals):
        mean = sums / entries
        variance = squares / entries - mean * mean
        factor = lax.rsqrt(variance + EPSILON) * gain
        result.append((factor, shift - mean * factor))
    return result


def normalized(values, terms):
    factor, offset = terms
    return (values * factor + offset).astype(BF16)


def kernel(strips, refs, in_sem):
    (f2, f3, f4, f5, w2, w3, w4, w5, bias, smooth, gain, shift) = refs[:12]
    outs = {0: refs[12], 2: refs[13], 3: refs[14], 4: refs[16]}
    cv3 = refs[15]
    norms = refs[17]
    cv2 = refs[18]
    (
        f2v, f3v, f4v, f5v, w2v, w3v, w4v, w5v, biasv, smv, gainv, shiftv,
        xc2, xc3, xc4, xc5,
        t2, t3, t4,
        lat3, lat4,
        e5, e4, e3,
        r5, r4, r3, r2,
        rb2, rb3, rb4, rb5,
        cv4, cv5,
        stats,
        sendA, sendB, recvA, recvB,
        edge_send, edge_recv, all_send, all_recv, entered,
    ) = refs[19:]
    current = []

    def phase(name):
        if current:
            current.pop().__exit__(None, None, None)
        if name:
            current.append(jax.named_scope(name))
            current[0].__enter__()

    phase("start")
    batch = lax.axis_index("batch")
    me = lax.axis_index("rows")
    peers = strips - 1
    above = lax.rem(me + strips - 1, strips)
    below = lax.rem(me + 1, strips)

    pairs = (
        (f4, f4v), (w4, w4v), (bias, biasv), (f5, f5v), (w5, w5v), (f3, f3v), (w3, w3v),
        (f2, f2v), (w2, w2v), (smooth.at[0], smv.at[0]), (smooth.at[1], smv.at[1]),
        (smooth.at[2], smv.at[2]), (smooth.at[3], smv.at[3]), (gain, gainv), (shift, shiftv),
    )
    loads = [pltpu.make_async_copy(s, d, in_sem.at[i]) for i, (s, d) in enumerate(pairs)]
    for load in loads:
        load.start()
    (lf4, lw4, lb, lf5, lw5, lf3, lw3, lf2, lw2, ls2, ls3, ls4, ls5, lg, lsh) = loads

    barrier = pltpu.get_barrier_semaphore()
    core = lax.rem(me, 2)
    x = lax.rem(lax.div(me, 2), SIDE)
    y = lax.div(me, 2 * SIDE)
    place = lambda j, i, c: (lax.rem(y + j, SIDE) * SIDE + lax.rem(x + i, SIDE)) * 2 + c
    partner = me + 1 - 2 * core
    nearest = [place(0, 1, core), place(0, SIDE - 1, core), place(1, 0, core), place(SIDE - 1, 0, core)]
    line = [place(0, i, core) for i in range(1, SIDE)]
    side = me + 2 * core - 1
    has_side = jnp.logical_and(side >= 0, side < strips)
    has_above = me > 0
    has_below = me < strips - 1

    def greet(semaphore, peer):
        pl.semaphore_signal(semaphore, inc=1, device_id=(batch, peer), device_id_type=MESH)

    pl.when(has_side)(lambda: greet(barrier, side))
    for peer in nearest + [partner]:
        greet(barrier, peer)

    first = me == 0
    last = me == strips - 1
    keep_top = jnp.where(first, 0.0, 1.0)
    keep_bottom = jnp.where(last, 0.0, 1.0)
    top_far = jnp.where(first, 0.0, 0.25)
    top_near = jnp.where(first, 1.0, 0.75)
    bottom_far = jnp.where(last, 0.0, 0.25)
    bottom_near = jnp.where(last, 1.0, 0.75)

    phase("matrices")
    blocks = interpolation(
        64, 3,
        (
            ((0, 0.75), (1, 0.25)),
            ((0, top_far), (1, top_near)),
            ((1, bottom_near), (2, bottom_far)),
            ((1, 0.25), (2, 0.75)),
        ),
        128,
    )
    for i, block in enumerate(blocks):
        t4[64 * i : 64 * i + 64, :] = block
    blocks = interpolation(
        128, 4,
        (
            ((0, top_far), (1, top_near)),
            ((1, 0.75), (2, 0.25)),
            ((1, 0.25), (2, 0.75)),
            ((2, bottom_near), (3, bottom_far)),
            ((0, 0.75), (1, 0.25)),
            ((2, 0.25), (3, 0.75)),
        ),
        256,
    )
    for i, block in enumerate(blocks):
        t3[128 * i : 128 * i + 128, :] = block
    blocks = interpolation(
        256, 2,
        (
            ((0, 0.75), (1, 0.25)),
            ((0, 0.25), (1, 0.75)),
            ((0, top_far), (1, top_near)),
            ((0, bottom_near), (1, bottom_far)),
        ),
        256,
    )
    for place, which in ((0, 0), (1, 1), (2, 0), (3, 2), (4, 3), (5, 1)):
        t2[256 * place : 256 * place + 256, :] = blocks[which]

    for rb, cols in ((rb2, 256), (rb3, 128), (rb4, 64), (rb5, 32)):
        for copy in range(rb.shape[0]):
            for half in range(2):
                rb[copy, half, 0:8, :] = jnp.zeros((8, 128), F32)
                rb[copy, half, cols + 8 : cols + 16, :] = jnp.zeros((8, 128), F32)
    stats[...] = jnp.zeros_like(stats)

    def put_row(rb, copy, target, values):
        cols = values.shape[0]
        for half in range(2):
            rb[copy, half, 8 : 8 + cols, :] = values[:, 128 * half : 128 * half + 128]
        for half in range(2):
            target[2 + half] = values[:, 128 * half : 128 * half + 128].astype(BF16)
            for tap in (0, 2):
                target[2 * tap + half] = rb[copy, half, 7 + tap : 7 + tap + cols, :].astype(BF16)

    def middle(xc, image, row, rows):
        halves = [xc[image, row : row + rows, 2 + half] for half in range(2)]
        return jnp.concatenate([h.reshape(-1, 128) for h in halves], 1)

    def dot(a, b):
        return jnp.dot(a, b, preferred_element_type=F32)

    def edge(level, side, source, target, peer):
        return pltpu.make_async_remote_copy(
            src_ref=source,
            dst_ref=target,
            send_sem=edge_send.at[level, side],
            recv_sem=edge_recv.at[level, side],
            device_id=(batch, peer),
            device_id_type=MESH,
        )

    edges5 = (edge(3, 0, e5, r5.at[1], above), edge(3, 1, e5, r5.at[0], below))
    edges4 = (edge(2, 0, e4.at[0], r4.at[1], above), edge(2, 1, e4.at[1], r4.at[0], below))
    edges3 = (edge(1, 0, e3.at[0], r3.at[1], above), edge(1, 1, e3.at[1], r3.at[0], below))
    edges2 = (
        edge(0, 0, f2v.at[:, 0], r2.at[1], above),
        edge(0, 1, f2v.at[:, 7], r2.at[0], below),
    )

    def send(*levels):
        @pl.when(has_above)
        def _():
            for pair_of in levels:
                pair_of[0].start()

        @pl.when(has_below)
        def _():
            for pair_of in levels:
                pair_of[1].start()

    def receive(*levels):
        @pl.when(has_below)
        def _():
            for pair_of in levels:
                pair_of[0].wait_recv()

        @pl.when(has_above)
        def _():
            for pair_of in levels:
                pair_of[1].wait_recv()

    for side, missing in ((0, first), (1, last)):

        @pl.when(missing)
        def _():
            for halo in (r5, r4, r3, r2):
                halo[side] = jnp.zeros_like(halo[side])

    phase("wait_load4")
    lf4.wait()
    lw4.wait()
    lb.wait()
    phase("lat4")
    for image in range(IMAGES):
        flat = dot(f4v[image].reshape(128, 1024), w4v[...]) + biasv[2:3, :]
        for row in range(2):
            part = flat[row * 64 : row * 64 + 64]
            e4[row, image] = part.astype(BF16)
            lat4[image, row] = part
    phase("barrier")
    pl.semaphore_wait(barrier, 5 + jnp.where(has_side, 1, 0))
    send(edges4)
    phase("wait_load5")
    lf5.wait()
    lw5.wait()
    phase("lat5")
    merged = dot(f5v[...].reshape(64, 2048), w5v[...]) + biasv[3:4, :]
    e5[...] = merged.reshape(2, 32, 256).astype(BF16)
    for image in range(IMAGES):
        put_row(rb5, image, xc5.at[image, 1], merged[32 * image : 32 * image + 32])
    send(edges5)
    for peer in nearest + [partner]:
        greet(entered.at[0], peer)

    phase("wait_load3")
    lf3.wait()
    lw3.wait()
    phase("lat3")
    for image in range(IMAGES):
        flat = dot(f3v[image].reshape(512, 512), w3v[...]) + biasv[1:2, :]
        e3[0, image] = flat[0:128].astype(BF16)
        e3[1, image] = flat[384:512].astype(BF16)
        lat3[image] = flat
    send(edges3)
    phase("wait_load2")
    lf2.wait()
    send(edges2)

    phase("lat2")
    lw2.wait()

    @pl.loop(0, IMAGES)
    def _(image):
        for part in range(2):
            cv2[image, 1024 * part : 1024 * part + 1024, :] = (
                dot(f2v[image, 4 * part : 4 * part + 4].reshape(1024, 256), w2v[...])
                + biasv[0:1, :]
            )
    ls2.wait()
    ls4.wait()
    ls5.wait()

    phase("wait_edge5")
    receive(edges5, edges4)
    pl.semaphore_wait(entered.at[0], 5)
    for peer in line:
        greet(entered.at[1], peer)
    phase("merge")
    def pair(image, p, weights):
        return dot(weights, middle(xc3, image, p + 1, 2))

    def halo_five(image):
        put_row(rb5, 2 + image, xc5.at[image, 0], r5[0, image].astype(F32) * keep_top)
        put_row(rb5, 4 + image, xc5.at[image, 2], r5[1, image].astype(F32) * keep_bottom)

    def merge_four(image):
        coarse = jnp.concatenate([middle(xc5, image, 0, 3), jnp.zeros((32, 256), BF16)], 0)
        up = dot(t4[...], coarse)
        base = 4 * image
        put_row(rb4, base, xc4.at[image, 0], (up[0:64] + r4[0, image].astype(F32)) * keep_top)
        put_row(rb4, base + 1, xc4.at[image, 1], up[64:128] + lat4[image, 0])
        put_row(rb4, base + 2, xc4.at[image, 2], up[128:192] + lat4[image, 1])
        put_row(
            rb4, base + 3, xc4.at[image, 3], (up[192:256] + r4[1, image].astype(F32)) * keep_bottom
        )

    def merge_three(image):
        up = dot(t3[0:512, :], middle(xc4, image, 0, 4)) + lat3[image]
        for row in range(4):
            put_row(rb3, 4 * image + row, xc3.at[image, 1 + row], up[128 * row : 128 * row + 128])

    def merge_middle(image):
        for p in range(3):
            both = pair(image, p, t2[0:512, :])
            for row in range(2):
                start = 512 * p + 256 + 256 * row
                put_row(
                    rb2, 6 * image + 2 * p + row, xc2.at[image, 2 * p + 2 + row],
                    both[256 * row : 256 * row + 256] + cv2[image, start : start + 256, :],
                )

    def tally(level, image, values):
        tiles = values.reshape(values.shape[0] // 8, 8, 256)
        stats[level, image, 0] += jnp.sum(tiles, axis=0)
        stats[level, image, 1] += jnp.sum(tiles * tiles, axis=0)

    def product(bands, level):
        total = None
        for tap, slabs in enumerate(bands):
            term = dot(jnp.concatenate(slabs, 1), smv[level, tap])
            total = term if total is None else total + term
        return total

    def conv(xc, level, image, row, rows):
        return product(
            [
                [xc[image, row + tap : row + tap + rows, slab].reshape(-1, 128) for slab in range(6)]
                for tap in range(3)
            ],
            level,
        )

    def conv_two(image, row):
        values = conv(xc2, 0, image, row, 2)
        cv2[image, row * 256 : row * 256 + 512, :] = values
        tally(0, image, values)

    for stage in (halo_five, merge_four, merge_three):
        for image in range(IMAGES):
            stage(image)
    for image in range(IMAGES):
        merge_middle(image)
        for row in (2, 4):
            conv_two(image, row)

    values = product(
        [[xc5[:, tap, slab].reshape(64, 128) for slab in range(6)] for tap in range(3)], 3
    )
    cv5[...] = values
    for image in range(IMAGES):
        tally(3, image, values[32 * image : 32 * image + 32])
    values = product(
        [
            [xc4[:, tap : tap + 2, slab].reshape(256, 128) for slab in range(6)]
            for tap in range(3)
        ],
        2,
    )
    cv4[...] = values
    for image in range(IMAGES):
        tally(2, image, values[128 * image : 128 * image + 128])

    def conv_three(row, rows):
        for image in range(IMAGES):
            values = conv(xc3, 1, image, row, rows)
            cv3[image, 128 * row : 128 * (row + rows)] = values
            tally(1, image, values)

    phase("wait_edge3")
    receive(edges3, edges2)
    pl.semaphore_wait(entered.at[1], 3)
    greet(entered.at[2], partner)
    ls3.wait()
    phase("rest2")
    for image in range(IMAGES):
        up = dot(t3[512:768, :], middle(xc4, image, 0, 4))
        put_row(rb3, 8 + image, xc3.at[image, 0], (up[0:128] + r3[0, image].astype(F32)) * keep_top)
        put_row(rb3, 10 + image, xc3.at[image, 5], (up[128:256] + r3[1, image].astype(F32)) * keep_bottom)
    def merge_ends(image):
        both = pair(image, -1, t2[512:1024, :])
        outside = dot(r2[0, image], w2v[...]) + biasv[0:1, :]
        base = 12 + 4 * image
        put_row(rb2, base, xc2.at[image, 0], (both[0:256] + outside) * keep_top)
        put_row(rb2, base + 1, xc2.at[image, 1], both[256:512] + cv2[image, 0:256, :])
        both = pair(image, 3, t2[1024:1536, :])
        outside = dot(r2[1, image], w2v[...]) + biasv[0:1, :]
        put_row(rb2, base + 2, xc2.at[image, 8], both[0:256] + cv2[image, 1792:2048, :])
        put_row(rb2, base + 3, xc2.at[image, 9], (both[256:512] + outside) * keep_bottom)

    for image in range(IMAGES):
        merge_ends(image)
        for row in (0, 6):
            conv_two(image, row)

    conv_three(1, 2)

    def everyone(source, target, which):
        far = lambda i: min(i, SIDE - i)
        moves = sorted(
            ((j, i, c) for j in range(SIDE) for i in range(SIDE) for c in range(2) if i or j or c),
            key=lambda m: (-far(m[0]) - far(m[1]), m),
        )
        along = [2 * lax.rem(x + i, SIDE) for i in range(SIDE)]
        across = [2 * SIDE * lax.rem(y + j, SIDE) for j in range(SIDE)]
        cores = [core, 1 - core]
        return [
            pltpu.make_async_remote_copy(
                src_ref=source,
                dst_ref=target.at[slot],
                send_sem=all_send.at[which],
                recv_sem=all_recv.at[which],
                device_id=(batch, across[j] + along[i] + cores[c]),
                device_id_type=MESH,
            )
            for slot, (j, i, c) in enumerate(moves)
        ]

    phase("encodeA")
    sendA[...] = jnp.concatenate(
        [encode(stats.at[0]), encode(stats.at[2]), encode(stats.at[3]), jnp.zeros((1, 128), F32)], 0
    )
    pl.semaphore_wait(entered.at[2], 1)
    for copy in everyone(sendA, recvA, 0):
        copy.start()

    phase("conv3")
    for row in (0, 3):
        conv_three(row, 1)

    phase("encodeB")
    sendB[...] = encode(stats.at[1])
    for copy in everyone(sendB, recvB, 1):
        copy.start()

    lg.wait()
    lsh.wait()
    norms[0:1, :] = gainv[1:2, :]
    norms[1:2, :] = shiftv[1:2, :]
    def finish(level, totals):
        affine = affine_of(level, strips, totals, gainv[level : level + 1], shiftv[level : level + 1])
        for image, terms in enumerate(affine):
            if level == 0 and image == 0:

                @pl.loop(0, 4)
                def _(rows):
                    values = normalized(cv2[0, pl.ds(rows * 512, 512), :], terms)
                    outs[0][0, pl.ds(rows * 2, 2)] = values.reshape(2, 256, 256)

            elif level == 0:
                norms[2:3, :], norms[3:4, :] = terms
            else:
                if level == 2:
                    values = cv4[128 * image : 128 * image + 128]
                else:
                    values = cv5[32 * image : 32 * image + 32]
                outs[level][image] = normalized(values, terms).reshape(
                    STRIP[level], COLS[level], 256
                )

    phase("wait_A")
    pltpu.make_async_copy(recvA, recvA, all_recv.at[0]).wait()
    phase("normA")
    totals = sendA[...] + jnp.sum(recvA[...], axis=0)
    finish(0, totals[0:1])
    finish(2, totals[1:2])
    finish(3, totals[2:3])

    phase("wait_sends")
    @pl.when(has_above)
    def _():
        for pair_of in (edges5, edges4, edges3, edges2):
            pair_of[0].wait_send()

    @pl.when(has_below)
    def _():
        for pair_of in (edges5, edges4, edges3, edges2):
            pair_of[1].wait_send()

    pltpu.make_async_copy(recvA, recvA, all_send.at[0]).wait()
    pltpu.make_async_copy(recvB, recvB, all_send.at[1]).wait()
    phase("wait_B")
    pltpu.make_async_copy(recvB, recvB, all_recv.at[1]).wait()
    phase("normB")
    outs[4][...] = sendB[...] + jnp.sum(recvB[...], axis=0)
    phase(None)


def write_out(
    strips, in2, in4, in5, values, totals, norms, values2, out2, out3, out4, out5, made2, made3, sems
):
    pairs = [(in2, out2.at[pl.ds(0, 1)]), (in4, out4), (in5, out5)]
    pairs += [(made2.at[pl.ds(4 * j, 4)], out2.at[1, pl.ds(4 * j, 4)]) for j in range(2)]
    pairs += [(made3, out3)]
    copies = [pltpu.make_async_copy(*pair, sems.at[k]) for k, pair in enumerate(pairs)]
    for copy in copies[:3]:
        copy.start()
    terms = (norms[2:3, :], norms[3:4, :])
    for j in range(2):
        rows = normalized(values2[1, 1024 * j : 1024 * j + 1024, :], terms)
        made2[4 * j : 4 * j + 4] = rows.reshape(4, COLS[0], CHANNELS)
        copies[3 + j].start()
    affine = affine_of(1, strips, totals[...], norms[0:1, :], norms[1:2, :])
    for image, terms in enumerate(affine):
        made3[image] = normalized(values[image], terms).reshape(STRIP[1], COLS[1], CHANNELS)
    copies[5].start()
    for copy in copies:
        copy.wait()


def solution(mesh):
    strips = mesh.shape["rows"]

    def per_device(*args):
        vmem = pltpu.VMEM
        scratch = [
            vmem((2, 8, 256, 256), BF16), vmem((2, 4, 128, 512), BF16),
            vmem((2, 2, 64, 1024), BF16), vmem((2, 1, 32, 2048), BF16),
            vmem((256, 256), BF16), vmem((512, 256), BF16),
            vmem((1024, 256), BF16), vmem((2048, 256), BF16),
            vmem((4, 256), F32), vmem((4, 3, 768, 256), BF16),
            vmem((4, 256), F32), vmem((4, 256), F32),
            vmem((2, 10, 6, 256, 128), BF16), vmem((2, 6, 6, 128, 128), BF16),
            vmem((2, 4, 6, 64, 128), BF16), vmem((2, 3, 6, 32, 128), BF16),
            vmem((1536, 256), BF16), vmem((768, 256), BF16), vmem((256, 128), BF16),
            vmem((2, 512, 256), F32), vmem((2, 2, 64, 256), F32),
            vmem((2, 32, 256), BF16), vmem((2, 2, 64, 256), BF16), vmem((2, 2, 128, 256), BF16),
            vmem((2, 2, 32, 256), BF16), vmem((2, 2, 64, 256), BF16),
            vmem((2, 2, 128, 256), BF16), vmem((2, 2, 256, 256), BF16),
            vmem((20, 2, 272, 128), F32), vmem((12, 2, 144, 128), F32),
            vmem((8, 2, 80, 128), F32), vmem((6, 2, 48, 128), F32),
            vmem((256, 256), F32), vmem((64, 256), F32),
            vmem((4, 2, 2, 8, 256), F32),
            vmem((4, 128), F32), vmem((1, 128), F32),
            vmem((strips - 1, 4, 128), F32), vmem((strips - 1, 1, 128), F32),
            pltpu.SemaphoreType.DMA((4, 2)), pltpu.SemaphoreType.DMA((4, 2)),
            pltpu.SemaphoreType.DMA((2,)), pltpu.SemaphoreType.DMA((2,)),
            pltpu.SemaphoreType.REGULAR((3,)),
        ]
        results = pl.pallas_call(
            lambda *refs: pl.run_scoped(
                lambda in_sem: kernel(strips, refs, in_sem), pltpu.SemaphoreType.DMA((15,))
            ),
            name="pyramid",
            out_shape=[
                pltpu.VMEM((1 if k == 0 else IMAGES, STRIP[k], COLS[k], CHANNELS), BF16)
                for k in (0, 2, 3)
            ]
            + [
                pltpu.VMEM((IMAGES, STRIP[1] * COLS[1], CHANNELS), F32),
                pltpu.VMEM((1, 128), F32),
                pltpu.VMEM((4, CHANNELS), F32),
                pltpu.VMEM((IMAGES, STRIP[0] * COLS[0], CHANNELS), F32),
            ],
            in_specs=[pl.BlockSpec(memory_space=pltpu.HBM)] * 12,
            out_specs=[pl.BlockSpec(memory_space=pltpu.VMEM)] * 7,
            scratch_shapes=scratch,
            compiler_params=pltpu.CompilerParams(
                collective_id=0, has_side_effects=True, vmem_limit_bytes=48 << 20
            ),
            cost_estimate=pl.CostEstimate(
                flops=7_430_000_000, bytes_accessed=13_300_000, transcendentals=0
            ),
        )(*(pltpu.with_memory_space_constraint(a, pltpu.HBM) for a in args))
        return tuple(
            pl.pallas_call(
                lambda *refs: write_out(strips, *refs),
                name="write",
                out_shape=[
                    jax.ShapeDtypeStruct((IMAGES, STRIP[k], COLS[k], CHANNELS), BF16)
                    for k in range(4)
                ],
                in_specs=[pl.BlockSpec(memory_space=pltpu.VMEM)] * 7,
                out_specs=[pl.BlockSpec(memory_space=pltpu.HBM)] * 4,
                scratch_shapes=[
                    pltpu.VMEM((STRIP[0], COLS[0], CHANNELS), BF16),
                    pltpu.VMEM((IMAGES, STRIP[1], COLS[1], CHANNELS), BF16),
                    pltpu.SemaphoreType.DMA((6,)),
                ],
                compiler_params=pltpu.CompilerParams(vmem_limit_bytes=8 << 20),
                cost_estimate=pl.CostEstimate(
                    flops=0, bytes_accessed=5_600_000, transcendentals=0
                ),
            )(*(pltpu.with_memory_space_constraint(r, pltpu.VMEM) for r in results))
        )

    rows = P("batch", "rows", None, None)
    return jax.shard_map(
        per_device,
        mesh=mesh,
        in_specs=(rows,) * 4 + (P(),) * 8,
        out_specs=(rows,) * 4,
        check_vma=False,
    )
```

```python
import jax
import jax.numpy as jnp
from jax import lax
from jax.experimental import pallas as pl
from jax.experimental.pallas import tpu as pltpu
from jax.sharding import PartitionSpec as P

MESH = pl.DeviceIdType.MESH
F32 = jnp.float32
BF16 = jnp.bfloat16
EPSILON = 1e-05
CHANNELS = 256
GROUP = 8
IMAGES = 2
COLS = (256, 128, 64, 32)
STRIP = (8, 4, 2, 1)
DEPTH = (256, 512, 1024, 2048)
SIDE = 4


def interpolation(cols, coarse_rows, pieces, width):
    coarse = cols // 2
    lanes = lax.broadcasted_iota(jnp.int32, (cols, width), 1)
    fine = lax.broadcasted_iota(jnp.int32, (cols, width), 0)
    block = lax.div(lanes, coarse)
    column = lax.rem(lanes, coarse)
    near = lax.div(fine, 2)
    far = jnp.clip(near + 2 * lax.rem(fine, 2) - 1, 0, coarse - 1)
    taps = jnp.where(column == near, 0.75, 0.0) + jnp.where(column == far, 0.25, 0.0)
    result = []
    for pairs in pieces:
        weight = jnp.zeros((cols, width), F32)
        for row, value in pairs:
            weight = jnp.where(block == row, value, weight)
        result.append((taps * weight).astype(BF16))
    return result


def lane_groups(values):
    lane = lax.broadcasted_iota(jnp.int32, values.shape, 1)
    for step in (1, 2, 4):
        upper = lax.rem(lax.div(lane, step), 2) == 1
        values = values + jnp.where(
            upper, pltpu.roll(values, step, axis=1), pltpu.roll(values, 128 - step, axis=1)
        )
    return values


def encode(stats):
    rows = [
        jnp.sum(stats[image, kind], axis=0, keepdims=True)
        for image in range(IMAGES)
        for kind in range(2)
    ]
    packed = jnp.concatenate([r[:, :128] for r in rows] + [r[:, 128:] for r in rows], 0)
    packed = lane_groups(packed)
    lane = lax.broadcasted_iota(jnp.int32, packed.shape, 1)
    which = lax.broadcasted_iota(jnp.int32, packed.shape, 0)
    return jnp.sum(jnp.where(lax.rem(lane, 8) == which, packed, 0.0), axis=0, keepdims=True)


def decode(totals):
    spread = jnp.broadcast_to(totals, (8, 128))
    lane = lax.broadcasted_iota(jnp.int32, spread.shape, 1)
    which = lax.broadcasted_iota(jnp.int32, spread.shape, 0)
    spread = lane_groups(jnp.where(lax.rem(lane, 8) == which, spread, 0.0))
    row = lambda q: jnp.concatenate([spread[q : q + 1], spread[q + 4 : q + 5]], 1)
    return [(row(2 * image), row(2 * image + 1)) for image in range(IMAGES)]


def affine_of(level, strips, totals, gain, shift):
    entries = float(COLS[level] * strips * STRIP[level] * GROUP)
    result = []
    for sums, squares in decode(totals):
        mean = sums / entries
        variance = squares / entries - mean * mean
        factor = lax.rsqrt(variance + EPSILON) * gain
        result.append((factor, shift - mean * factor))
    return result


def normalized(values, terms):
    factor, offset = terms
    return (values * factor + offset).astype(BF16)


def kernel(strips, refs, in_sem):
    (f2, f3, f4, f5, w2, w3, w4, w5, bias, smooth, gain, shift) = refs[:12]
    outs = {0: refs[12], 2: refs[13], 3: refs[14], 4: refs[16]}
    cv3 = refs[15]
    norms = refs[17]
    cv2 = refs[18]
    (
        f2v, f3v, f4v, f5v, w2v, w3v, w4v, w5v, biasv, smv, gainv, shiftv,
        xc2, xc3, xc4, xc5,
        t2, t3, t4,
        lat3, lat4,
        e5, e4, e3,
        r5, r4, r3, r2,
        rb2, rb3, rb4, rb5,
        cv4, cv5,
        stats,
        sendA, sendB, recvA, recvB,
        edge_send, edge_recv, all_send, all_recv, entered,
    ) = refs[19:]
    current = []

    def phase(name):
        if current:
            current.pop().__exit__(None, None, None)
        if name:
            current.append(jax.named_scope(name))
            current[0].__enter__()

    phase("start")
    batch = lax.axis_index("batch")
    me = lax.axis_index("rows")
    peers = strips - 1
    above = lax.rem(me + strips - 1, strips)
    below = lax.rem(me + 1, strips)

    pairs = (
        (f4, f4v), (w4, w4v), (bias, biasv), (f5, f5v), (w5, w5v), (f3, f3v), (w3, w3v),
        (f2, f2v), (w2, w2v), (smooth.at[0], smv.at[0]), (smooth.at[1], smv.at[1]),
        (smooth.at[2], smv.at[2]), (smooth.at[3], smv.at[3]), (gain, gainv), (shift, shiftv),
    )
    loads = [pltpu.make_async_copy(s, d, in_sem.at[i]) for i, (s, d) in enumerate(pairs)]
    for load in loads:
        load.start()
    (lf4, lw4, lb, lf5, lw5, lf3, lw3, lf2, lw2, ls2, ls3, ls4, ls5, lg, lsh) = loads

    barrier = pltpu.get_barrier_semaphore()
    core = lax.rem(me, 2)
    x = lax.rem(lax.div(me, 2), SIDE)
    y = lax.div(me, 2 * SIDE)
    place = lambda j, i, c: (lax.rem(y + j, SIDE) * SIDE + lax.rem(x + i, SIDE)) * 2 + c
    partner = me + 1 - 2 * core
    nearest = [place(0, 1, core), place(0, SIDE - 1, core), place(1, 0, core), place(SIDE - 1, 0, core)]
    line = [place(0, i, core) for i in range(1, SIDE)]
    side = me + 2 * core - 1
    has_side = jnp.logical_and(side >= 0, side < strips)
    has_above = me > 0
    has_below = me < strips - 1

    def greet(semaphore, peer):
        pl.semaphore_signal(semaphore, inc=1, device_id=(batch, peer), device_id_type=MESH)

    pl.when(has_side)(lambda: greet(barrier, side))
    for peer in nearest + [partner]:
        greet(barrier, peer)

    first = me == 0
    last = me == strips - 1
    keep_top = jnp.where(first, 0.0, 1.0)
    keep_bottom = jnp.where(last, 0.0, 1.0)
    top_far = jnp.where(first, 0.0, 0.25)
    top_near = jnp.where(first, 1.0, 0.75)
    bottom_far = jnp.where(last, 0.0, 0.25)
    bottom_near = jnp.where(last, 1.0, 0.75)

    phase("matrices")
    blocks = interpolation(
        64, 3,
        (
            ((0, 0.75), (1, 0.25)),
            ((0, top_far), (1, top_near)),
            ((1, bottom_near), (2, bottom_far)),
            ((1, 0.25), (2, 0.75)),
        ),
        128,
    )
    for i, block in enumerate(blocks):
        t4[64 * i : 64 * i + 64, :] = block
    blocks = interpolation(
        128, 4,
        (
            ((0, top_far), (1, top_near)),
            ((1, 0.75), (2, 0.25)),
            ((1, 0.25), (2, 0.75)),
            ((2, bottom_near), (3, bottom_far)),
            ((0, 0.75), (1, 0.25)),
            ((2, 0.25), (3, 0.75)),
        ),
        256,
    )
    for i, block in enumerate(blocks):
        t3[128 * i : 128 * i + 128, :] = block
    blocks = interpolation(
        256, 2,
        (
            ((0, 0.75), (1, 0.25)),
            ((0, 0.25), (1, 0.75)),
            ((0, top_far), (1, top_near)),
            ((0, bottom_near), (1, bottom_far)),
        ),
        256,
    )
    for place, which in ((0, 0), (1, 1), (2, 0), (3, 2), (4, 3), (5, 1)):
        t2[256 * place : 256 * place + 256, :] = blocks[which]

    for rb, cols in ((rb2, 256), (rb3, 128), (rb4, 64), (rb5, 32)):
        for copy in range(rb.shape[0]):
            for half in range(2):
                rb[copy, half, 0:8, :] = jnp.zeros((8, 128), F32)
                rb[copy, half, cols + 8 : cols + 16, :] = jnp.zeros((8, 128), F32)
    stats[...] = jnp.zeros_like(stats)

    def put_row(rb, copy, target, values):
        cols = values.shape[0]
        for half in range(2):
            rb[copy, half, 8 : 8 + cols, :] = values[:, 128 * half : 128 * half + 128]
        for half in range(2):
            target[2 + half] = values[:, 128 * half : 128 * half + 128].astype(BF16)
            for tap in (0, 2):
                target[2 * tap + half] = rb[copy, half, 7 + tap : 7 + tap + cols, :].astype(BF16)

    def middle(xc, image, row, rows):
        halves = [xc[image, row : row + rows, 2 + half] for half in range(2)]
        return jnp.concatenate([h.reshape(-1, 128) for h in halves], 1)

    def dot(a, b):
        return jnp.dot(a, b, preferred_element_type=F32)

    def edge(level, side, source, target, peer):
        return pltpu.make_async_remote_copy(
            src_ref=source,
            dst_ref=target,
            send_sem=edge_send.at[level, side],
            recv_sem=edge_recv.at[level, side],
            device_id=(batch, peer),
            device_id_type=MESH,
        )

    edges5 = (edge(3, 0, e5, r5.at[1], above), edge(3, 1, e5, r5.at[0], below))
    edges4 = (edge(2, 0, e4.at[0], r4.at[1], above), edge(2, 1, e4.at[1], r4.at[0], below))
    edges3 = (edge(1, 0, e3.at[0], r3.at[1], above), edge(1, 1, e3.at[1], r3.at[0], below))
    edges2 = (
        edge(0, 0, f2v.at[:, 0], r2.at[1], above),
        edge(0, 1, f2v.at[:, 7], r2.at[0], below),
    )

    def send(*levels):
        @pl.when(has_above)
        def _():
            for pair_of in levels:
                pair_of[0].start()

        @pl.when(has_below)
        def _():
            for pair_of in levels:
                pair_of[1].start()

    def receive(*levels):
        @pl.when(has_below)
        def _():
            for pair_of in levels:
                pair_of[0].wait_recv()

        @pl.when(has_above)
        def _():
            for pair_of in levels:
                pair_of[1].wait_recv()

    for side, missing in ((0, first), (1, last)):

        @pl.when(missing)
        def _():
            for halo in (r5, r4, r3, r2):
                halo[side] = jnp.zeros_like(halo[side])

    phase("wait_load4")
    lf4.wait()
    lw4.wait()
    lb.wait()
    phase("lat4")
    for image in range(IMAGES):
        flat = dot(f4v[image].reshape(128, 1024), w4v[...]) + biasv[2:3, :]
        for row in range(2):
            part = flat[row * 64 : row * 64 + 64]
            e4[row, image] = part.astype(BF16)
            lat4[image, row] = part
    phase("barrier")
    pl.semaphore_wait(barrier, 5 + jnp.where(has_side, 1, 0))
    send(edges4)
    phase("wait_load5")
    lf5.wait()
    lw5.wait()
    phase("lat5")
    merged = dot(f5v[...].reshape(64, 2048), w5v[...]) + biasv[3:4, :]
    e5[...] = merged.reshape(2, 32, 256).astype(BF16)
    for image in range(IMAGES):
        put_row(rb5, image, xc5.at[image, 1], merged[32 * image : 32 * image + 32])
    send(edges5)
    for peer in nearest + [partner]:
        greet(entered.at[0], peer)

    phase("wait_load3")
    lf3.wait()
    lw3.wait()
    phase("lat3")
    for image in range(IMAGES):
        flat = dot(f3v[image].reshape(512, 512), w3v[...]) + biasv[1:2, :]
        e3[0, image] = flat[0:128].astype(BF16)
        e3[1, image] = flat[384:512].astype(BF16)
        lat3[image] = flat
    send(edges3)
    phase("wait_load2")
    lf2.wait()
    send(edges2)

    phase("lat2")
    lw2.wait()

    @pl.loop(0, IMAGES)
    def _(image):
        for part in range(2):
            cv2[image, 1024 * part : 1024 * part + 1024, :] = (
                dot(f2v[image, 4 * part : 4 * part + 4].reshape(1024, 256), w2v[...])
                + biasv[0:1, :]
            )
    ls2.wait()
    ls4.wait()
    ls5.wait()

    phase("wait_edge5")
    receive(edges5, edges4)
    pl.semaphore_wait(entered.at[0], 5)
    for peer in line:
        greet(entered.at[1], peer)
    phase("merge")
    def pair(image, p, weights):
        return dot(weights, middle(xc3, image, p + 1, 2))

    def halo_five(image):
        put_row(rb5, 2 + image, xc5.at[image, 0], r5[0, image].astype(F32) * keep_top)
        put_row(rb5, 4 + image, xc5.at[image, 2], r5[1, image].astype(F32) * keep_bottom)

    def merge_four(image):
        coarse = jnp.concatenate([middle(xc5, image, 0, 3), jnp.zeros((32, 256), BF16)], 0)
        up = dot(t4[...], coarse)
        base = 4 * image
        put_row(rb4, base, xc4.at[image, 0], (up[0:64] + r4[0, image].astype(F32)) * keep_top)
        put_row(rb4, base + 1, xc4.at[image, 1], up[64:128] + lat4[image, 0])
        put_row(rb4, base + 2, xc4.at[image, 2], up[128:192] + lat4[image, 1])
        put_row(
            rb4, base + 3, xc4.at[image, 3], (up[192:256] + r4[1, image].astype(F32)) * keep_bottom
        )

    def merge_three(image):
        up = dot(t3[0:512, :], middle(xc4, image, 0, 4)) + lat3[image]
        for row in range(4):
            put_row(rb3, 4 * image + row, xc3.at[image, 1 + row], up[128 * row : 128 * row + 128])

    def merge_middle(image):
        for p in range(3):
            both = pair(image, p, t2[0:512, :])
            for row in range(2):
                start = 512 * p + 256 + 256 * row
                put_row(
                    rb2, 6 * image + 2 * p + row, xc2.at[image, 2 * p + 2 + row],
                    both[256 * row : 256 * row + 256] + cv2[image, start : start + 256, :],
                )

    def tally(level, image, values):
        tiles = values.reshape(values.shape[0] // 8, 8, 256)
        stats[level, image, 0] += jnp.sum(tiles, axis=0)
        stats[level, image, 1] += jnp.sum(tiles * tiles, axis=0)

    def product(bands, level):
        total = None
        for tap, slabs in enumerate(bands):
            term = dot(jnp.concatenate(slabs, 1), smv[level, tap])
            total = term if total is None else total + term
        return total

    def conv(xc, level, image, row, rows):
        return product(
            [
                [xc[image, row + tap : row + tap + rows, slab].reshape(-1, 128) for slab in range(6)]
                for tap in range(3)
            ],
            level,
        )

    def conv_two(image, row):
        values = conv(xc2, 0, image, row, 2)
        cv2[image, row * 256 : row * 256 + 512, :] = values
        tally(0, image, values)

    def conv_five():
        values = product(
            [[xc5[:, tap, slab].reshape(64, 128) for slab in range(6)] for tap in range(3)], 3
        )
        cv5[...] = values
        for image in range(IMAGES):
            tally(3, image, values[32 * image : 32 * image + 32])

    def conv_four():
        values = product(
            [
                [xc4[:, tap : tap + 2, slab].reshape(256, 128) for slab in range(6)]
                for tap in range(3)
            ],
            2,
        )
        cv4[...] = values
        for image in range(IMAGES):
            tally(2, image, values[128 * image : 128 * image + 128])


    for image in range(IMAGES):
        halo_five(image)
    for image in range(IMAGES):
        merge_four(image)
    conv_five()
    for image in range(IMAGES):
        merge_three(image)
    conv_four()
    for image in range(IMAGES):
        merge_middle(image)
    for image in range(IMAGES):
        for row in (2, 4):
            conv_two(image, row)


    def conv_three(row, rows):
        for image in range(IMAGES):
            values = conv(xc3, 1, image, row, rows)
            cv3[image, 128 * row : 128 * (row + rows)] = values
            tally(1, image, values)

    phase("wait_edge3")
    receive(edges3, edges2)
    pl.semaphore_wait(entered.at[1], 3)
    greet(entered.at[2], partner)
    ls3.wait()
    phase("rest2")
    for image in range(IMAGES):
        up = dot(t3[512:768, :], middle(xc4, image, 0, 4))
        put_row(rb3, 8 + image, xc3.at[image, 0], (up[0:128] + r3[0, image].astype(F32)) * keep_top)
        put_row(rb3, 10 + image, xc3.at[image, 5], (up[128:256] + r3[1, image].astype(F32)) * keep_bottom)
    def merge_ends(image):
        both = pair(image, -1, t2[512:1024, :])
        outside = dot(r2[0, image], w2v[...]) + biasv[0:1, :]
        base = 12 + 4 * image
        put_row(rb2, base, xc2.at[image, 0], (both[0:256] + outside) * keep_top)
        put_row(rb2, base + 1, xc2.at[image, 1], both[256:512] + cv2[image, 0:256, :])
        both = pair(image, 3, t2[1024:1536, :])
        outside = dot(r2[1, image], w2v[...]) + biasv[0:1, :]
        put_row(rb2, base + 2, xc2.at[image, 8], both[0:256] + cv2[image, 1792:2048, :])
        put_row(rb2, base + 3, xc2.at[image, 9], (both[256:512] + outside) * keep_bottom)

    conv_three(1, 2)
    for image in range(IMAGES):
        merge_ends(image)
    for image in range(IMAGES):
        for row in (0, 6):
            conv_two(image, row)

    def everyone(source, target, which):
        far = lambda i: min(i, SIDE - i)
        moves = sorted(
            ((j, i, c) for j in range(SIDE) for i in range(SIDE) for c in range(2) if i or j or c),
            key=lambda m: (-far(m[0]) - far(m[1]), m),
        )
        along = [2 * lax.rem(x + i, SIDE) for i in range(SIDE)]
        across = [2 * SIDE * lax.rem(y + j, SIDE) for j in range(SIDE)]
        cores = [core, 1 - core]
        return [
            pltpu.make_async_remote_copy(
                src_ref=source,
                dst_ref=target.at[slot],
                send_sem=all_send.at[which],
                recv_sem=all_recv.at[which],
                device_id=(batch, across[j] + along[i] + cores[c]),
                device_id_type=MESH,
            )
            for slot, (j, i, c) in enumerate(moves)
        ]

    phase("encodeA")
    sendA[...] = jnp.concatenate(
        [encode(stats.at[0]), encode(stats.at[2]), encode(stats.at[3]), jnp.zeros((1, 128), F32)], 0
    )
    pl.semaphore_wait(entered.at[2], 1)
    for copy in everyone(sendA, recvA, 0):
        copy.start()

    phase("conv3")
    for image in range(IMAGES):
        values = product(
            [
                [
                    jnp.concatenate([xc3[image, row + tap, slab] for row in (0, 3)], 0)
                    for slab in range(6)
                ]
                for tap in range(3)
            ],
            1,
        )
        cv3[image, 0:128] = values[0:128]
        cv3[image, 384:512] = values[128:256]
        tally(1, image, values)

    phase("encodeB")
    sendB[...] = encode(stats.at[1])
    for copy in everyone(sendB, recvB, 1):
        copy.start()

    lg.wait()
    lsh.wait()
    norms[0:1, :] = gainv[1:2, :]
    norms[1:2, :] = shiftv[1:2, :]
    def finish(level, totals):
        affine = affine_of(level, strips, totals, gainv[level : level + 1], shiftv[level : level + 1])
        for image, terms in enumerate(affine):
            if level == 0 and image == 0:

                @pl.loop(0, 4)
                def _(rows):
                    values = normalized(cv2[0, pl.ds(rows * 512, 512), :], terms)
                    outs[0][0, pl.ds(rows * 2, 2)] = values.reshape(2, 256, 256)

            elif level == 0:
                norms[2:3, :], norms[3:4, :] = terms
            else:
                if level == 2:
                    values = cv4[128 * image : 128 * image + 128]
                else:
                    values = cv5[32 * image : 32 * image + 32]
                outs[level][image] = normalized(values, terms).reshape(
                    STRIP[level], COLS[level], 256
                )

    phase("wait_A")
    pltpu.make_async_copy(recvA, recvA, all_recv.at[0]).wait()
    phase("normA")
    totals = sendA[...] + jnp.sum(recvA[...], axis=0)
    finish(0, totals[0:1])
    finish(2, totals[1:2])
    finish(3, totals[2:3])

    phase("wait_sends")
    @pl.when(has_above)
    def _():
        for pair_of in (edges5, edges4, edges3, edges2):
            pair_of[0].wait_send()

    @pl.when(has_below)
    def _():
        for pair_of in (edges5, edges4, edges3, edges2):
            pair_of[1].wait_send()

    pltpu.make_async_copy(recvA, recvA, all_send.at[0]).wait()
    pltpu.make_async_copy(recvB, recvB, all_send.at[1]).wait()
    phase("wait_B")
    pltpu.make_async_copy(recvB, recvB, all_recv.at[1]).wait()
    phase("normB")
    outs[4][...] = sendB[...] + jnp.sum(recvB[...], axis=0)
    phase(None)


def write_out(
    strips, in2, in4, in5, values, totals, norms, values2, out2, out3, out4, out5, made2, made3, sems
):
    pairs = [(in2, out2.at[pl.ds(0, 1)]), (in4, out4), (in5, out5)]
    pairs += [(made2.at[pl.ds(4 * j, 4)], out2.at[1, pl.ds(4 * j, 4)]) for j in range(2)]
    pairs += [(made3, out3)]
    copies = [pltpu.make_async_copy(*pair, sems.at[k]) for k, pair in enumerate(pairs)]
    for copy in copies[:3]:
        copy.start()
    terms = (norms[2:3, :], norms[3:4, :])
    for j in range(2):
        rows = normalized(values2[1, 1024 * j : 1024 * j + 1024, :], terms)
        made2[4 * j : 4 * j + 4] = rows.reshape(4, COLS[0], CHANNELS)
        copies[3 + j].start()
    affine = affine_of(1, strips, totals[...], norms[0:1, :], norms[1:2, :])
    for image, terms in enumerate(affine):
        made3[image] = normalized(values[image], terms).reshape(STRIP[1], COLS[1], CHANNELS)
    copies[5].start()
    for copy in copies:
        copy.wait()


def solution(mesh):
    strips = mesh.shape["rows"]

    def per_device(*args):
        vmem = pltpu.VMEM
        scratch = [
            vmem((2, 8, 256, 256), BF16), vmem((2, 4, 128, 512), BF16),
            vmem((2, 2, 64, 1024), BF16), vmem((2, 1, 32, 2048), BF16),
            vmem((256, 256), BF16), vmem((512, 256), BF16),
            vmem((1024, 256), BF16), vmem((2048, 256), BF16),
            vmem((4, 256), F32), vmem((4, 3, 768, 256), BF16),
            vmem((4, 256), F32), vmem((4, 256), F32),
            vmem((2, 10, 6, 256, 128), BF16), vmem((2, 6, 6, 128, 128), BF16),
            vmem((2, 4, 6, 64, 128), BF16), vmem((2, 3, 6, 32, 128), BF16),
            vmem((1536, 256), BF16), vmem((768, 256), BF16), vmem((256, 128), BF16),
            vmem((2, 512, 256), F32), vmem((2, 2, 64, 256), F32),
            vmem((2, 32, 256), BF16), vmem((2, 2, 64, 256), BF16), vmem((2, 2, 128, 256), BF16),
            vmem((2, 2, 32, 256), BF16), vmem((2, 2, 64, 256), BF16),
            vmem((2, 2, 128, 256), BF16), vmem((2, 2, 256, 256), BF16),
            vmem((20, 2, 272, 128), F32), vmem((12, 2, 144, 128), F32),
            vmem((8, 2, 80, 128), F32), vmem((6, 2, 48, 128), F32),
            vmem((256, 256), F32), vmem((64, 256), F32),
            vmem((4, 2, 2, 8, 256), F32),
            vmem((4, 128), F32), vmem((1, 128), F32),
            vmem((strips - 1, 4, 128), F32), vmem((strips - 1, 1, 128), F32),
            pltpu.SemaphoreType.DMA((4, 2)), pltpu.SemaphoreType.DMA((4, 2)),
            pltpu.SemaphoreType.DMA((2,)), pltpu.SemaphoreType.DMA((2,)),
            pltpu.SemaphoreType.REGULAR((3,)),
        ]
        results = pl.pallas_call(
            lambda *refs: pl.run_scoped(
                lambda in_sem: kernel(strips, refs, in_sem), pltpu.SemaphoreType.DMA((15,))
            ),
            name="pyramid",
            out_shape=[
                pltpu.VMEM((1 if k == 0 else IMAGES, STRIP[k], COLS[k], CHANNELS), BF16)
                for k in (0, 2, 3)
            ]
            + [
                pltpu.VMEM((IMAGES, STRIP[1] * COLS[1], CHANNELS), F32),
                pltpu.VMEM((1, 128), F32),
                pltpu.VMEM((4, CHANNELS), F32),
                pltpu.VMEM((IMAGES, STRIP[0] * COLS[0], CHANNELS), F32),
            ],
            in_specs=[pl.BlockSpec(memory_space=pltpu.HBM)] * 12,
            out_specs=[pl.BlockSpec(memory_space=pltpu.VMEM)] * 7,
            scratch_shapes=scratch,
            compiler_params=pltpu.CompilerParams(
                collective_id=0, has_side_effects=True, vmem_limit_bytes=48 << 20
            ),
            cost_estimate=pl.CostEstimate(
                flops=7_430_000_000, bytes_accessed=13_300_000, transcendentals=0
            ),
        )(*(pltpu.with_memory_space_constraint(a, pltpu.HBM) for a in args))
        return tuple(
            pl.pallas_call(
                lambda *refs: write_out(strips, *refs),
                name="write",
                out_shape=[
                    jax.ShapeDtypeStruct((IMAGES, STRIP[k], COLS[k], CHANNELS), BF16)
                    for k in range(4)
                ],
                in_specs=[pl.BlockSpec(memory_space=pltpu.VMEM)] * 7,
                out_specs=[pl.BlockSpec(memory_space=pltpu.HBM)] * 4,
                scratch_shapes=[
                    pltpu.VMEM((STRIP[0], COLS[0], CHANNELS), BF16),
                    pltpu.VMEM((IMAGES, STRIP[1], COLS[1], CHANNELS), BF16),
                    pltpu.SemaphoreType.DMA((6,)),
                ],
                compiler_params=pltpu.CompilerParams(vmem_limit_bytes=8 << 20),
                cost_estimate=pl.CostEstimate(
                    flops=0, bytes_accessed=5_600_000, transcendentals=0
                ),
            )(*(pltpu.with_memory_space_constraint(r, pltpu.VMEM) for r in results))
        )

    rows = P("batch", "rows", None, None)
    return jax.shard_map(
        per_device,
        mesh=mesh,
        in_specs=(rows,) * 4 + (P(),) * 8,
        out_specs=(rows,) * 4,
        check_vma=False,
    )
```

```python
import jax
import jax.numpy as jnp
from jax import lax
from jax.experimental import pallas as pl
from jax.experimental.pallas import tpu as pltpu
from jax.sharding import PartitionSpec as P

MESH = pl.DeviceIdType.MESH
F32 = jnp.float32
BF16 = jnp.bfloat16
EPSILON = 1e-05
CHANNELS = 256
GROUP = 8
IMAGES = 2
COLS = (256, 128, 64, 32)
STRIP = (8, 4, 2, 1)
DEPTH = (256, 512, 1024, 2048)
SIDE = 4


def interpolation(cols, coarse_rows, pieces, width):
    coarse = cols // 2
    lanes = lax.broadcasted_iota(jnp.int32, (cols, width), 1)
    fine = lax.broadcasted_iota(jnp.int32, (cols, width), 0)
    block = lax.div(lanes, coarse)
    column = lax.rem(lanes, coarse)
    near = lax.div(fine, 2)
    far = jnp.clip(near + 2 * lax.rem(fine, 2) - 1, 0, coarse - 1)
    taps = jnp.where(column == near, 0.75, 0.0) + jnp.where(column == far, 0.25, 0.0)
    result = []
    for pairs in pieces:
        weight = jnp.zeros((cols, width), F32)
        for row, value in pairs:
            weight = jnp.where(block == row, value, weight)
        result.append((taps * weight).astype(BF16))
    return result


def lane_groups(values):
    lane = lax.broadcasted_iota(jnp.int32, values.shape, 1)
    for step in (1, 2, 4):
        upper = lax.rem(lax.div(lane, step), 2) == 1
        values = values + jnp.where(
            upper, pltpu.roll(values, step, axis=1), pltpu.roll(values, 128 - step, axis=1)
        )
    return values


def encode(stats):
    rows = [
        jnp.sum(stats[image, kind], axis=0, keepdims=True)
        for image in range(IMAGES)
        for kind in range(2)
    ]
    packed = jnp.concatenate([r[:, :128] for r in rows] + [r[:, 128:] for r in rows], 0)
    packed = lane_groups(packed)
    lane = lax.broadcasted_iota(jnp.int32, packed.shape, 1)
    which = lax.broadcasted_iota(jnp.int32, packed.shape, 0)
    return jnp.sum(jnp.where(lax.rem(lane, 8) == which, packed, 0.0), axis=0, keepdims=True)


def decode(totals):
    spread = jnp.broadcast_to(totals, (8, 128))
    lane = lax.broadcasted_iota(jnp.int32, spread.shape, 1)
    which = lax.broadcasted_iota(jnp.int32, spread.shape, 0)
    spread = lane_groups(jnp.where(lax.rem(lane, 8) == which, spread, 0.0))
    row = lambda q: jnp.concatenate([spread[q : q + 1], spread[q + 4 : q + 5]], 1)
    return [(row(2 * image), row(2 * image + 1)) for image in range(IMAGES)]


def affine_of(level, strips, totals, gain, shift):
    entries = float(COLS[level] * strips * STRIP[level] * GROUP)
    result = []
    for sums, squares in decode(totals):
        mean = sums / entries
        variance = squares / entries - mean * mean
        factor = lax.rsqrt(variance + EPSILON) * gain
        result.append((factor, shift - mean * factor))
    return result


def normalized(values, terms):
    factor, offset = terms
    return (values * factor + offset).astype(BF16)


def kernel(strips, refs, in_sem, edge_send, edge_recv, all_send, all_recv, entered):
    (f2, f3, f4, f5, w2, w3, w4, w5, bias, smooth, gain, shift) = refs[:12]
    outs = {0: refs[12], 2: refs[13], 3: refs[14], 4: refs[16]}
    cv3 = refs[15]
    norms = refs[17]
    cv2 = refs[18]
    (
        f2v, f3v, f4v, f5v, w2v, w3v, w4v, w5v, biasv, smv, gainv, shiftv,
        xc2, xc3, xc4, xc5,
        t2, t3, t4,
        lat3, lat4,
        e5, e4, e3,
        r5, r4, r3, r2,
        rb2, rb3, rb4, rb5,
        cv4, cv5,
        stats,
        sendA, sendB, recvA, recvB,
    ) = refs[19:]
    current = []

    def phase(name):
        if current:
            current.pop().__exit__(None, None, None)
        if name:
            current.append(jax.named_scope(name))
            current[0].__enter__()

    phase("start")
    batch = lax.axis_index("batch")
    me = lax.axis_index("rows")
    peers = strips - 1
    above = lax.rem(me + strips - 1, strips)
    below = lax.rem(me + 1, strips)

    pairs = (
        (f4, f4v), (w4, w4v), (bias, biasv), (f5, f5v), (w5, w5v), (f3, f3v), (w3, w3v),
        (f2, f2v), (w2, w2v), (smooth.at[0], smv.at[0]), (smooth.at[1], smv.at[1]),
        (smooth.at[2], smv.at[2]), (smooth.at[3], smv.at[3]), (gain, gainv), (shift, shiftv),
    )
    loads = [pltpu.make_async_copy(s, d, in_sem.at[i]) for i, (s, d) in enumerate(pairs)]
    for load in loads:
        load.start()
    (lf4, lw4, lb, lf5, lw5, lf3, lw3, lf2, lw2, ls2, ls3, ls4, ls5, lg, lsh) = loads

    barrier = pltpu.get_barrier_semaphore()
    core = lax.rem(me, 2)
    x = lax.rem(lax.div(me, 2), SIDE)
    y = lax.div(me, 2 * SIDE)
    place = lambda j, i, c: (lax.rem(y + j, SIDE) * SIDE + lax.rem(x + i, SIDE)) * 2 + c
    partner = me + 1 - 2 * core
    nearest = [place(0, 1, core), place(0, SIDE - 1, core), place(1, 0, core), place(SIDE - 1, 0, core)]
    line = [place(0, i, core) for i in range(1, SIDE)]
    side = me + 2 * core - 1
    has_side = jnp.logical_and(side >= 0, side < strips)
    has_above = me > 0
    has_below = me < strips - 1

    def greet(semaphore, peer):
        pl.semaphore_signal(semaphore, inc=1, device_id=(batch, peer), device_id_type=MESH)

    pl.when(has_side)(lambda: greet(barrier, side))
    for peer in nearest + [partner]:
        greet(barrier, peer)

    first = me == 0
    last = me == strips - 1
    keep_top = jnp.where(first, 0.0, 1.0)
    keep_bottom = jnp.where(last, 0.0, 1.0)
    top_far = jnp.where(first, 0.0, 0.25)
    top_near = jnp.where(first, 1.0, 0.75)
    bottom_far = jnp.where(last, 0.0, 0.25)
    bottom_near = jnp.where(last, 1.0, 0.75)

    phase("matrices")
    blocks = interpolation(
        64, 3,
        (
            ((0, 0.75), (1, 0.25)),
            ((0, top_far), (1, top_near)),
            ((1, bottom_near), (2, bottom_far)),
            ((1, 0.25), (2, 0.75)),
        ),
        128,
    )
    for i, block in enumerate(blocks):
        t4[64 * i : 64 * i + 64, :] = block
    blocks = interpolation(
        128, 4,
        (
            ((0, top_far), (1, top_near)),
            ((1, 0.75), (2, 0.25)),
            ((1, 0.25), (2, 0.75)),
            ((2, bottom_near), (3, bottom_far)),
            ((0, 0.75), (1, 0.25)),
            ((2, 0.25), (3, 0.75)),
        ),
        256,
    )
    for i, block in enumerate(blocks):
        t3[128 * i : 128 * i + 128, :] = block
    blocks = interpolation(
        256, 2,
        (
            ((0, 0.75), (1, 0.25)),
            ((0, 0.25), (1, 0.75)),
            ((0, top_far), (1, top_near)),
            ((0, bottom_near), (1, bottom_far)),
        ),
        256,
    )
    for place, which in ((0, 0), (1, 1), (2, 0), (3, 2), (4, 3), (5, 1)):
        t2[256 * place : 256 * place + 256, :] = blocks[which]

    for rb, cols in ((rb2, 256), (rb3, 128), (rb4, 64), (rb5, 32)):
        for copy in range(rb.shape[0]):
            for half in range(2):
                rb[copy, half, 0:8, :] = jnp.zeros((8, 128), F32)
                rb[copy, half, cols + 8 : cols + 16, :] = jnp.zeros((8, 128), F32)
    stats[...] = jnp.zeros_like(stats)

    def put_row(rb, copy, target, values):
        cols = values.shape[0]
        for half in range(2):
            rb[copy, half, 8 : 8 + cols, :] = values[:, 128 * half : 128 * half + 128]
        for half in range(2):
            target[2 + half] = values[:, 128 * half : 128 * half + 128].astype(BF16)
            for tap in (0, 2):
                target[2 * tap + half] = rb[copy, half, 7 + tap : 7 + tap + cols, :].astype(BF16)

    def middle(xc, image, row, rows):
        halves = [xc[image, row : row + rows, 2 + half] for half in range(2)]
        return jnp.concatenate([h.reshape(-1, 128) for h in halves], 1)

    def dot(a, b):
        return jnp.dot(a, b, preferred_element_type=F32)

    def edge(level, side, source, target, peer):
        return pltpu.make_async_remote_copy(
            src_ref=source,
            dst_ref=target,
            send_sem=edge_send.at[level, side],
            recv_sem=edge_recv.at[level, side],
            device_id=(batch, peer),
            device_id_type=MESH,
        )

    edges5 = (edge(3, 0, e5, r5.at[1], above), edge(3, 1, e5, r5.at[0], below))
    edges4 = (edge(2, 0, e4.at[0], r4.at[1], above), edge(2, 1, e4.at[1], r4.at[0], below))
    edges3 = (edge(1, 0, e3.at[0], r3.at[1], above), edge(1, 1, e3.at[1], r3.at[0], below))
    edges2 = (
        edge(0, 0, f2v.at[:, 0], r2.at[1], above),
        edge(0, 1, f2v.at[:, 7], r2.at[0], below),
    )

    def send(*levels):
        @pl.when(has_above)
        def _():
            for pair_of in levels:
                pair_of[0].start()

        @pl.when(has_below)
        def _():
            for pair_of in levels:
                pair_of[1].start()

    def receive(*levels):
        @pl.when(has_below)
        def _():
            for pair_of in levels:
                pair_of[0].wait_recv()

        @pl.when(has_above)
        def _():
            for pair_of in levels:
                pair_of[1].wait_recv()

    for side, missing in ((0, first), (1, last)):

        @pl.when(missing)
        def _():
            for halo in (r5, r4, r3, r2):
                halo[side] = jnp.zeros_like(halo[side])

    phase("wait_load4")
    lf4.wait()
    lw4.wait()
    lb.wait()
    phase("lat4")
    for image in range(IMAGES):
        flat = dot(f4v[image].reshape(128, 1024), w4v[...]) + biasv[2:3, :]
        for row in range(2):
            part = flat[row * 64 : row * 64 + 64]
            e4[row, image] = part.astype(BF16)
            lat4[image, row] = part
    phase("barrier")
    pl.semaphore_wait(barrier, 5 + jnp.where(has_side, 1, 0))
    send(edges4)
    phase("wait_load5")
    lf5.wait()
    lw5.wait()
    phase("lat5")
    merged = dot(f5v[...].reshape(64, 2048), w5v[...]) + biasv[3:4, :]
    e5[...] = merged.reshape(2, 32, 256).astype(BF16)
    for image in range(IMAGES):
        put_row(rb5, image, xc5.at[image, 1], merged[32 * image : 32 * image + 32])
    send(edges5)
    for peer in nearest + [partner]:
        greet(entered.at[0], peer)

    phase("wait_load3")
    lf3.wait()
    lw3.wait()
    phase("lat3")
    for image in range(IMAGES):
        flat = dot(f3v[image].reshape(512, 512), w3v[...]) + biasv[1:2, :]
        e3[0, image] = flat[0:128].astype(BF16)
        e3[1, image] = flat[384:512].astype(BF16)
        lat3[image] = flat
    send(edges3)
    phase("wait_load2")
    lf2.wait()
    send(edges2)

    phase("lat2")
    lw2.wait()

    @pl.loop(0, IMAGES)
    def _(image):
        for part in range(2):
            cv2[image, 1024 * part : 1024 * part + 1024, :] = (
                dot(f2v[image, 4 * part : 4 * part + 4].reshape(1024, 256), w2v[...])
                + biasv[0:1, :]
            )
    ls2.wait()
    ls4.wait()
    ls5.wait()

    phase("wait_edge5")
    receive(edges5, edges4)
    pl.semaphore_wait(entered.at[0], 5)
    for peer in line:
        greet(entered.at[1], peer)
    phase("merge")
    def pair(image, p, weights):
        return dot(weights, middle(xc3, image, p + 1, 2))

    def halo_five(image):
        put_row(rb5, 2 + image, xc5.at[image, 0], r5[0, image].astype(F32) * keep_top)
        put_row(rb5, 4 + image, xc5.at[image, 2], r5[1, image].astype(F32) * keep_bottom)

    def merge_four(image):
        coarse = jnp.concatenate([middle(xc5, image, 0, 3), jnp.zeros((32, 256), BF16)], 0)
        up = dot(t4[...], coarse)
        base = 4 * image
        put_row(rb4, base, xc4.at[image, 0], (up[0:64] + r4[0, image].astype(F32)) * keep_top)
        put_row(rb4, base + 1, xc4.at[image, 1], up[64:128] + lat4[image, 0])
        put_row(rb4, base + 2, xc4.at[image, 2], up[128:192] + lat4[image, 1])
        put_row(
            rb4, base + 3, xc4.at[image, 3], (up[192:256] + r4[1, image].astype(F32)) * keep_bottom
        )

    def merge_three(image):
        up = dot(t3[0:512, :], middle(xc4, image, 0, 4)) + lat3[image]
        for row in range(4):
            put_row(rb3, 4 * image + row, xc3.at[image, 1 + row], up[128 * row : 128 * row + 128])

    def merge_middle(image):
        for p in range(3):
            both = pair(image, p, t2[0:512, :])
            for row in range(2):
                start = 512 * p + 256 + 256 * row
                put_row(
                    rb2, 6 * image + 2 * p + row, xc2.at[image, 2 * p + 2 + row],
                    both[256 * row : 256 * row + 256] + cv2[image, start : start + 256, :],
                )

    def tally(level, image, values):
        tiles = values.reshape(values.shape[0] // 8, 8, 256)
        stats[level, image, 0] += jnp.sum(tiles, axis=0)
        stats[level, image, 1] += jnp.sum(tiles * tiles, axis=0)

    def product(bands, level):
        total = None
        for tap, slabs in enumerate(bands):
            term = dot(jnp.concatenate(slabs, 1), smv[level, tap])
            total = term if total is None else total + term
        return total

    def conv(xc, level, image, row, rows):
        return product(
            [
                [xc[image, row + tap : row + tap + rows, slab].reshape(-1, 128) for slab in range(6)]
                for tap in range(3)
            ],
            level,
        )

    def conv_two(image, row):
        values = conv(xc2, 0, image, row, 2)
        cv2[image, row * 256 : row * 256 + 512, :] = values
        tally(0, image, values)

    def conv_five():
        values = product(
            [[xc5[:, tap, slab].reshape(64, 128) for slab in range(6)] for tap in range(3)], 3
        )
        cv5[...] = values
        for image in range(IMAGES):
            tally(3, image, values[32 * image : 32 * image + 32])

    def conv_four():
        values = product(
            [
                [xc4[:, tap : tap + 2, slab].reshape(256, 128) for slab in range(6)]
                for tap in range(3)
            ],
            2,
        )
        cv4[...] = values
        for image in range(IMAGES):
            tally(2, image, values[128 * image : 128 * image + 128])


    for image in range(IMAGES):
        halo_five(image)
    for image in range(IMAGES):
        merge_four(image)
    conv_five()
    for image in range(IMAGES):
        merge_three(image)
    conv_four()
    for image in range(IMAGES):
        merge_middle(image)
    for image in range(IMAGES):
        for row in (2, 4):
            conv_two(image, row)


    def conv_three(row, rows):
        for image in range(IMAGES):
            values = conv(xc3, 1, image, row, rows)
            cv3[image, 128 * row : 128 * (row + rows)] = values
            tally(1, image, values)

    phase("wait_edge3")
    receive(edges3, edges2)
    pl.semaphore_wait(entered.at[1], 3)
    greet(entered.at[2], partner)
    ls3.wait()
    phase("rest2")
    for image in range(IMAGES):
        up = dot(t3[512:768, :], middle(xc4, image, 0, 4))
        put_row(rb3, 8 + image, xc3.at[image, 0], (up[0:128] + r3[0, image].astype(F32)) * keep_top)
        put_row(rb3, 10 + image, xc3.at[image, 5], (up[128:256] + r3[1, image].astype(F32)) * keep_bottom)
    def merge_ends(image):
        both = pair(image, -1, t2[512:1024, :])
        outside = dot(r2[0, image], w2v[...]) + biasv[0:1, :]
        base = 12 + 4 * image
        put_row(rb2, base, xc2.at[image, 0], (both[0:256] + outside) * keep_top)
        put_row(rb2, base + 1, xc2.at[image, 1], both[256:512] + cv2[image, 0:256, :])
        both = pair(image, 3, t2[1024:1536, :])
        outside = dot(r2[1, image], w2v[...]) + biasv[0:1, :]
        put_row(rb2, base + 2, xc2.at[image, 8], both[0:256] + cv2[image, 1792:2048, :])
        put_row(rb2, base + 3, xc2.at[image, 9], (both[256:512] + outside) * keep_bottom)

    conv_three(1, 2)
    for image in range(IMAGES):
        merge_ends(image)
    for image in range(IMAGES):
        for row in (0, 6):
            conv_two(image, row)

    def everyone(source, target, which):
        far = lambda i: min(i, SIDE - i)
        moves = sorted(
            ((j, i, c) for j in range(SIDE) for i in range(SIDE) for c in range(2) if i or j or c),
            key=lambda m: (-far(m[0]) - far(m[1]), m),
        )
        along = [2 * lax.rem(x + i, SIDE) for i in range(SIDE)]
        across = [2 * SIDE * lax.rem(y + j, SIDE) for j in range(SIDE)]
        cores = [core, 1 - core]
        return [
            pltpu.make_async_remote_copy(
                src_ref=source,
                dst_ref=target.at[slot],
                send_sem=all_send.at[which],
                recv_sem=all_recv.at[which],
                device_id=(batch, across[j] + along[i] + cores[c]),
                device_id_type=MESH,
            )
            for slot, (j, i, c) in enumerate(moves)
        ]

    phase("encodeA")
    sendA[...] = jnp.concatenate(
        [encode(stats.at[0]), encode(stats.at[2]), encode(stats.at[3]), jnp.zeros((1, 128), F32)], 0
    )
    pl.semaphore_wait(entered.at[2], 1)
    for copy in everyone(sendA, recvA, 0):
        copy.start()

    phase("conv3")
    for image in range(IMAGES):
        values = product(
            [
                [
                    jnp.concatenate([xc3[image, row + tap, slab] for row in (0, 3)], 0)
                    for slab in range(6)
                ]
                for tap in range(3)
            ],
            1,
        )
        cv3[image, 0:128] = values[0:128]
        cv3[image, 384:512] = values[128:256]
        tally(1, image, values)

    phase("encodeB")
    sendB[...] = encode(stats.at[1])
    for copy in everyone(sendB, recvB, 1):
        copy.start()

    lg.wait()
    lsh.wait()
    norms[0:1, :] = gainv[1:2, :]
    norms[1:2, :] = shiftv[1:2, :]
    def finish(level, totals):
        affine = affine_of(level, strips, totals, gainv[level : level + 1], shiftv[level : level + 1])
        for image, terms in enumerate(affine):
            if level == 0 and image == 0:

                @pl.loop(0, 4)
                def _(rows):
                    values = normalized(cv2[0, pl.ds(rows * 512, 512), :], terms)
                    outs[0][0, pl.ds(rows * 2, 2)] = values.reshape(2, 256, 256)

            elif level == 0:
                norms[2:3, :], norms[3:4, :] = terms
            else:
                if level == 2:
                    values = cv4[128 * image : 128 * image + 128]
                else:
                    values = cv5[32 * image : 32 * image + 32]
                outs[level][image] = normalized(values, terms).reshape(
                    STRIP[level], COLS[level], 256
                )

    phase("wait_A")
    pltpu.make_async_copy(recvA, recvA, all_recv.at[0]).wait()
    phase("normA")
    totals = sendA[...] + jnp.sum(recvA[...], axis=0)
    finish(0, totals[0:1])
    finish(2, totals[1:2])
    finish(3, totals[2:3])

    phase("wait_sends")
    @pl.when(has_above)
    def _():
        for pair_of in (edges5, edges4, edges3, edges2):
            pair_of[0].wait_send()

    @pl.when(has_below)
    def _():
        for pair_of in (edges5, edges4, edges3, edges2):
            pair_of[1].wait_send()

    pltpu.make_async_copy(recvA, recvA, all_send.at[0]).wait()
    pltpu.make_async_copy(recvB, recvB, all_send.at[1]).wait()
    phase("wait_B")
    pltpu.make_async_copy(recvB, recvB, all_recv.at[1]).wait()
    phase("normB")
    outs[4][...] = sendB[...] + jnp.sum(recvB[...], axis=0)
    phase(None)


def write_out(
    strips, in2, in4, in5, values, totals, norms, values2, out2, out3, out4, out5, made2, made3, sems
):
    pairs = [(in2, out2.at[pl.ds(0, 1)]), (in4, out4), (in5, out5)]
    pairs += [(made2.at[pl.ds(4 * j, 4)], out2.at[1, pl.ds(4 * j, 4)]) for j in range(2)]
    pairs += [(made3, out3)]
    copies = [pltpu.make_async_copy(*pair, sems.at[k]) for k, pair in enumerate(pairs)]
    for copy in copies[:3]:
        copy.start()
    terms = (norms[2:3, :], norms[3:4, :])
    for j in range(2):
        rows = normalized(values2[1, 1024 * j : 1024 * j + 1024, :], terms)
        made2[4 * j : 4 * j + 4] = rows.reshape(4, COLS[0], CHANNELS)
        copies[3 + j].start()
    affine = affine_of(1, strips, totals[...], norms[0:1, :], norms[1:2, :])
    for image, terms in enumerate(affine):
        made3[image] = normalized(values[image], terms).reshape(STRIP[1], COLS[1], CHANNELS)
    copies[5].start()
    for copy in copies:
        copy.wait()


def solution(mesh):
    strips = mesh.shape["rows"]

    def per_device(*args):
        vmem = pltpu.VMEM
        scratch = [
            vmem((2, 8, 256, 256), BF16), vmem((2, 4, 128, 512), BF16),
            vmem((2, 2, 64, 1024), BF16), vmem((2, 1, 32, 2048), BF16),
            vmem((256, 256), BF16), vmem((512, 256), BF16),
            vmem((1024, 256), BF16), vmem((2048, 256), BF16),
            vmem((4, 256), F32), vmem((4, 3, 768, 256), BF16),
            vmem((4, 256), F32), vmem((4, 256), F32),
            vmem((2, 10, 6, 256, 128), BF16), vmem((2, 6, 6, 128, 128), BF16),
            vmem((2, 4, 6, 64, 128), BF16), vmem((2, 3, 6, 32, 128), BF16),
            vmem((1536, 256), BF16), vmem((768, 256), BF16), vmem((256, 128), BF16),
            vmem((2, 512, 256), F32), vmem((2, 2, 64, 256), F32),
            vmem((2, 32, 256), BF16), vmem((2, 2, 64, 256), BF16), vmem((2, 2, 128, 256), BF16),
            vmem((2, 2, 32, 256), BF16), vmem((2, 2, 64, 256), BF16),
            vmem((2, 2, 128, 256), BF16), vmem((2, 2, 256, 256), BF16),
            vmem((20, 2, 272, 128), F32), vmem((12, 2, 144, 128), F32),
            vmem((8, 2, 80, 128), F32), vmem((6, 2, 48, 128), F32),
            vmem((256, 256), F32), vmem((64, 256), F32),
            vmem((4, 2, 2, 8, 256), F32),
            vmem((4, 128), F32), vmem((1, 128), F32),
            vmem((strips - 1, 4, 128), F32), vmem((strips - 1, 1, 128), F32),
        ]
        results = pl.pallas_call(
            lambda *refs: pl.run_scoped(
                lambda *semaphores: kernel(strips, refs, *semaphores),
                pltpu.SemaphoreType.DMA((15,)),
                pltpu.SemaphoreType.DMA((4, 2)),
                pltpu.SemaphoreType.DMA((4, 2)),
                pltpu.SemaphoreType.DMA((2,)),
                pltpu.SemaphoreType.DMA((2,)),
                pltpu.SemaphoreType.REGULAR((3,)),
            ),
            name="pyramid",
            out_shape=[
                pltpu.VMEM((1 if k == 0 else IMAGES, STRIP[k], COLS[k], CHANNELS), BF16)
                for k in (0, 2, 3)
            ]
            + [
                pltpu.VMEM((IMAGES, STRIP[1] * COLS[1], CHANNELS), F32),
                pltpu.VMEM((1, 128), F32),
                pltpu.VMEM((4, CHANNELS), F32),
                pltpu.VMEM((IMAGES, STRIP[0] * COLS[0], CHANNELS), F32),
            ],
            in_specs=[pl.BlockSpec(memory_space=pltpu.HBM)] * 12,
            out_specs=[pl.BlockSpec(memory_space=pltpu.VMEM)] * 7,
            scratch_shapes=scratch,
            compiler_params=pltpu.CompilerParams(
                collective_id=0, has_side_effects=True, vmem_limit_bytes=48 << 20
            ),
            cost_estimate=pl.CostEstimate(
                flops=7_430_000_000, bytes_accessed=13_300_000, transcendentals=0
            ),
        )(*(pltpu.with_memory_space_constraint(a, pltpu.HBM) for a in args))
        return tuple(
            pl.pallas_call(
                lambda *refs: pl.run_scoped(
                    lambda sems: write_out(strips, *refs, sems), pltpu.SemaphoreType.DMA((6,))
                ),
                name="write",
                out_shape=[
                    jax.ShapeDtypeStruct((IMAGES, STRIP[k], COLS[k], CHANNELS), BF16)
                    for k in range(4)
                ],
                in_specs=[pl.BlockSpec(memory_space=pltpu.VMEM)] * 7,
                out_specs=[pl.BlockSpec(memory_space=pltpu.HBM)] * 4,
                scratch_shapes=[
                    pltpu.VMEM((STRIP[0], COLS[0], CHANNELS), BF16),
                    pltpu.VMEM((IMAGES, STRIP[1], COLS[1], CHANNELS), BF16),
                ],
                compiler_params=pltpu.CompilerParams(vmem_limit_bytes=8 << 20),
                cost_estimate=pl.CostEstimate(
                    flops=0, bytes_accessed=5_600_000, transcendentals=0
                ),
            )(*(pltpu.with_memory_space_constraint(r, pltpu.VMEM) for r in results))
        )

    rows = P("batch", "rows", None, None)
    return jax.shard_map(
        per_device,
        mesh=mesh,
        in_specs=(rows,) * 4 + (P(),) * 8,
        out_specs=(rows,) * 4,
        check_vma=False,
    )
```

```python
import jax
import jax.numpy as jnp
from jax import lax
from jax.experimental import pallas as pl
from jax.experimental.pallas import tpu as pltpu
from jax.sharding import PartitionSpec as P

MESH = pl.DeviceIdType.MESH
F32 = jnp.float32
BF16 = jnp.bfloat16
EPSILON = 1e-05
CHANNELS = 256
GROUP = 8
IMAGES = 2
COLS = (256, 128, 64, 32)
STRIP = (8, 4, 2, 1)
DEPTH = (256, 512, 1024, 2048)
SIDE = 4


def interpolation(cols, coarse_rows, pieces, width):
    coarse = cols // 2
    lanes = lax.broadcasted_iota(jnp.int32, (cols, width), 1)
    fine = lax.broadcasted_iota(jnp.int32, (cols, width), 0)
    block = lax.div(lanes, coarse)
    column = lax.rem(lanes, coarse)
    near = lax.div(fine, 2)
    far = jnp.clip(near + 2 * lax.rem(fine, 2) - 1, 0, coarse - 1)
    taps = jnp.where(column == near, 0.75, 0.0) + jnp.where(column == far, 0.25, 0.0)
    result = []
    for pairs in pieces:
        weight = jnp.zeros((cols, width), F32)
        for row, value in pairs:
            weight = jnp.where(block == row, value, weight)
        result.append((taps * weight).astype(BF16))
    return result


def lane_groups(values):
    lane = lax.broadcasted_iota(jnp.int32, values.shape, 1)
    for step in (1, 2, 4):
        upper = lax.rem(lax.div(lane, step), 2) == 1
        values = values + jnp.where(
            upper, pltpu.roll(values, step, axis=1), pltpu.roll(values, 128 - step, axis=1)
        )
    return values


def encode(stats):
    rows = [
        jnp.sum(stats[image, kind], axis=0, keepdims=True)
        for image in range(IMAGES)
        for kind in range(2)
    ]
    packed = jnp.concatenate([r[:, :128] for r in rows] + [r[:, 128:] for r in rows], 0)
    packed = lane_groups(packed)
    lane = lax.broadcasted_iota(jnp.int32, packed.shape, 1)
    which = lax.broadcasted_iota(jnp.int32, packed.shape, 0)
    return jnp.sum(jnp.where(lax.rem(lane, 8) == which, packed, 0.0), axis=0, keepdims=True)


def decode(totals):
    spread = jnp.broadcast_to(totals, (8, 128))
    lane = lax.broadcasted_iota(jnp.int32, spread.shape, 1)
    which = lax.broadcasted_iota(jnp.int32, spread.shape, 0)
    spread = lane_groups(jnp.where(lax.rem(lane, 8) == which, spread, 0.0))
    row = lambda q: jnp.concatenate([spread[q : q + 1], spread[q + 4 : q + 5]], 1)
    return [(row(2 * image), row(2 * image + 1)) for image in range(IMAGES)]


def affine_of(level, strips, totals, gain, shift):
    entries = float(COLS[level] * strips * STRIP[level] * GROUP)
    result = []
    for sums, squares in decode(totals):
        mean = sums / entries
        variance = squares / entries - mean * mean
        factor = lax.rsqrt(variance + EPSILON) * gain
        result.append((factor, shift - mean * factor))
    return result


def normalized(values, terms):
    factor, offset = terms
    return (values * factor + offset).astype(BF16)


def kernel(strips, refs, in_sem, edge_send, edge_recv, all_send, all_recv, entered):
    (f2, f3, f4, f5, w2, w3, w4, w5, bias, smooth, gain, shift) = refs[:12]
    outs = {0: refs[12], 2: refs[13], 3: refs[14], 4: refs[16]}
    cv3 = refs[15]
    norms = refs[17]
    cv2 = refs[18]
    (
        f2v, f3v, f4v, f5v, w2v, w3v, w4v, w5v, biasv, smv, gainv, shiftv,
        xc2, xc3, xc4, xc5,
        t2, t3, t4,
        lat3, lat4,
        e5, e4, e3,
        r5, r4, r3, r2,
        rb2, rb3, rb4, rb5,
        cv4, cv5,
        stats,
        sendA, sendB, recvA, recvB,
    ) = refs[19:]
    current = []

    def phase(name):
        if current:
            current.pop().__exit__(None, None, None)
        if name:
            current.append(jax.named_scope(name))
            current[0].__enter__()

    phase("start")
    batch = lax.axis_index("batch")
    me = lax.axis_index("rows")
    peers = strips - 1
    above = lax.rem(me + strips - 1, strips)
    below = lax.rem(me + 1, strips)

    pairs = (
        (f4, f4v), (w4, w4v), (bias, biasv), (f5, f5v), (w5, w5v), (f3, f3v), (w3, w3v),
        (f2, f2v), (w2, w2v), (smooth.at[0], smv.at[0]), (smooth.at[1], smv.at[1]),
        (smooth.at[2], smv.at[2]), (smooth.at[3], smv.at[3]), (gain, gainv), (shift, shiftv),
    )
    loads = [pltpu.make_async_copy(s, d, in_sem.at[i]) for i, (s, d) in enumerate(pairs)]
    for load in loads:
        load.start()
    (lf4, lw4, lb, lf5, lw5, lf3, lw3, lf2, lw2, ls2, ls3, ls4, ls5, lg, lsh) = loads

    barrier = pltpu.get_barrier_semaphore()
    core = lax.rem(me, 2)
    x = lax.rem(lax.div(me, 2), SIDE)
    y = lax.div(me, 2 * SIDE)
    place = lambda j, i, c: (lax.rem(y + j, SIDE) * SIDE + lax.rem(x + i, SIDE)) * 2 + c
    partner = me + 1 - 2 * core
    nearest = [place(0, 1, core), place(0, SIDE - 1, core), place(1, 0, core), place(SIDE - 1, 0, core)]
    line = [place(0, i, core) for i in range(1, SIDE)]
    side = me + 2 * core - 1
    has_side = jnp.logical_and(side >= 0, side < strips)
    has_above = me > 0
    has_below = me < strips - 1

    def greet(semaphore, peer):
        pl.semaphore_signal(semaphore, inc=1, device_id=(batch, peer), device_id_type=MESH)

    pl.when(has_side)(lambda: greet(barrier, side))
    for peer in nearest + [partner]:
        greet(barrier, peer)

    first = me == 0
    last = me == strips - 1
    keep_top = jnp.where(first, 0.0, 1.0)
    keep_bottom = jnp.where(last, 0.0, 1.0)
    top_far = jnp.where(first, 0.0, 0.25)
    top_near = jnp.where(first, 1.0, 0.75)
    bottom_far = jnp.where(last, 0.0, 0.25)
    bottom_near = jnp.where(last, 1.0, 0.75)

    phase("matrices")
    blocks = interpolation(
        64, 3,
        (
            ((0, 0.75), (1, 0.25)),
            ((0, top_far), (1, top_near)),
            ((1, bottom_near), (2, bottom_far)),
            ((1, 0.25), (2, 0.75)),
        ),
        128,
    )
    for i, block in enumerate(blocks):
        t4[64 * i : 64 * i + 64, :] = block
    blocks = interpolation(
        128, 4,
        (
            ((0, top_far), (1, top_near)),
            ((1, 0.75), (2, 0.25)),
            ((1, 0.25), (2, 0.75)),
            ((2, bottom_near), (3, bottom_far)),
            ((0, 0.75), (1, 0.25)),
            ((2, 0.25), (3, 0.75)),
        ),
        256,
    )
    for i, block in enumerate(blocks):
        t3[128 * i : 128 * i + 128, :] = block
    blocks = interpolation(
        256, 2,
        (
            ((0, 0.75), (1, 0.25)),
            ((0, 0.25), (1, 0.75)),
            ((0, top_far), (1, top_near)),
            ((0, bottom_near), (1, bottom_far)),
        ),
        256,
    )
    for place, which in ((0, 0), (1, 1), (2, 0), (3, 2), (4, 3), (5, 1)):
        t2[256 * place : 256 * place + 256, :] = blocks[which]

    for rb, cols in ((rb2, 256), (rb3, 128), (rb4, 64), (rb5, 32)):
        for copy in range(rb.shape[0]):
            for half in range(2):
                rb[copy, half, 0:8, :] = jnp.zeros((8, 128), F32)
                rb[copy, half, cols + 8 : cols + 16, :] = jnp.zeros((8, 128), F32)
    stats[...] = jnp.zeros_like(stats)

    def put_row(rb, copy, target, values):
        cols = values.shape[0]
        for half in range(2):
            rb[copy, half, 8 : 8 + cols, :] = values[:, 128 * half : 128 * half + 128]
        for half in range(2):
            target[2 + half] = values[:, 128 * half : 128 * half + 128].astype(BF16)
            for tap in (0, 2):
                target[2 * tap + half] = rb[copy, half, 7 + tap : 7 + tap + cols, :].astype(BF16)

    def middle(xc, image, row, rows):
        halves = [xc[image, row : row + rows, 2 + half] for half in range(2)]
        return jnp.concatenate([h.reshape(-1, 128) for h in halves], 1)

    def dot(a, b):
        return jnp.dot(a, b, preferred_element_type=F32)

    def edge(level, side, source, target, peer):
        return pltpu.make_async_remote_copy(
            src_ref=source,
            dst_ref=target,
            send_sem=edge_send.at[level, side],
            recv_sem=edge_recv.at[level, side],
            device_id=(batch, peer),
            device_id_type=MESH,
        )

    edges5 = (edge(3, 0, e5, r5.at[1], above), edge(3, 1, e5, r5.at[0], below))
    edges4 = (edge(2, 0, e4.at[0], r4.at[1], above), edge(2, 1, e4.at[1], r4.at[0], below))
    edges3 = (edge(1, 0, e3.at[0], r3.at[1], above), edge(1, 1, e3.at[1], r3.at[0], below))
    edges2 = (
        edge(0, 0, f2v.at[:, 0], r2.at[1], above),
        edge(0, 1, f2v.at[:, 7], r2.at[0], below),
    )

    def send(*levels):
        @pl.when(has_above)
        def _():
            for pair_of in levels:
                pair_of[0].start()

        @pl.when(has_below)
        def _():
            for pair_of in levels:
                pair_of[1].start()

    def receive(*levels):
        @pl.when(has_below)
        def _():
            for pair_of in levels:
                pair_of[0].wait_recv()

        @pl.when(has_above)
        def _():
            for pair_of in levels:
                pair_of[1].wait_recv()

    for side, missing in ((0, first), (1, last)):

        @pl.when(missing)
        def _():
            for halo in (r5, r4, r3, r2):
                halo[side] = jnp.zeros_like(halo[side])

    phase("wait_load4")
    lf4.wait()
    lw4.wait()
    lb.wait()
    phase("lat4")
    for image in range(IMAGES):
        flat = dot(f4v[image].reshape(128, 1024), w4v[...]) + biasv[2:3, :]
        for row in range(2):
            part = flat[row * 64 : row * 64 + 64]
            e4[row, image] = part.astype(BF16)
            lat4[image, row] = part
    phase("barrier")
    pl.semaphore_wait(barrier, 5 + jnp.where(has_side, 1, 0))
    send(edges4)
    phase("wait_load5")
    lf5.wait()
    lw5.wait()
    phase("lat5")
    merged = dot(f5v[...].reshape(64, 2048), w5v[...]) + biasv[3:4, :]
    e5[...] = merged.reshape(2, 32, 256).astype(BF16)
    for image in range(IMAGES):
        put_row(rb5, image, xc5.at[image, 1], merged[32 * image : 32 * image + 32])
    send(edges5)
    for peer in nearest + [partner]:
        greet(entered.at[0], peer)

    phase("wait_load3")
    lf3.wait()
    lw3.wait()
    phase("lat3")
    for image in range(IMAGES):
        flat = dot(f3v[image].reshape(512, 512), w3v[...]) + biasv[1:2, :]
        e3[0, image] = flat[0:128].astype(BF16)
        e3[1, image] = flat[384:512].astype(BF16)
        lat3[image] = flat
    send(edges3)
    phase("wait_load2")
    lf2.wait()
    send(edges2)

    phase("lat2")
    lw2.wait()

    @pl.loop(0, IMAGES)
    def _(image):
        for part in range(2):
            cv2[image, 1024 * part : 1024 * part + 1024, :] = (
                dot(f2v[image, 4 * part : 4 * part + 4].reshape(1024, 256), w2v[...])
                + biasv[0:1, :]
            )
    ls2.wait()
    ls4.wait()
    ls5.wait()

    phase("wait_edge5")
    receive(edges5, edges4)
    pl.semaphore_wait(entered.at[0], 5)
    for peer in line:
        greet(entered.at[1], peer)
    phase("merge")
    def pair(image, p, weights):
        return dot(weights, middle(xc3, image, p + 1, 2))

    def halo_five(image):
        put_row(rb5, 2 + image, xc5.at[image, 0], r5[0, image].astype(F32) * keep_top)
        put_row(rb5, 4 + image, xc5.at[image, 2], r5[1, image].astype(F32) * keep_bottom)

    def merge_four(image):
        coarse = jnp.concatenate([middle(xc5, image, 0, 3), jnp.zeros((32, 256), BF16)], 0)
        up = dot(t4[...], coarse)
        base = 4 * image
        put_row(rb4, base, xc4.at[image, 0], (up[0:64] + r4[0, image].astype(F32)) * keep_top)
        put_row(rb4, base + 1, xc4.at[image, 1], up[64:128] + lat4[image, 0])
        put_row(rb4, base + 2, xc4.at[image, 2], up[128:192] + lat4[image, 1])
        put_row(
            rb4, base + 3, xc4.at[image, 3], (up[192:256] + r4[1, image].astype(F32)) * keep_bottom
        )

    def merge_three(image):
        up = dot(t3[0:512, :], middle(xc4, image, 0, 4)) + lat3[image]
        for row in range(4):
            put_row(rb3, 4 * image + row, xc3.at[image, 1 + row], up[128 * row : 128 * row + 128])

    def merge_middle(image):
        for p in range(3):
            both = pair(image, p, t2[0:512, :])
            for row in range(2):
                start = 512 * p + 256 + 256 * row
                put_row(
                    rb2, 6 * image + 2 * p + row, xc2.at[image, 2 * p + 2 + row],
                    both[256 * row : 256 * row + 256] + cv2[image, start : start + 256, :],
                )

    def tally(level, image, values):
        tiles = values.reshape(values.shape[0] // 8, 8, 256)
        stats[level, image, 0] += jnp.sum(tiles, axis=0)
        stats[level, image, 1] += jnp.sum(tiles * tiles, axis=0)

    def product(bands, level):
        total = None
        for tap, slabs in enumerate(bands):
            term = dot(jnp.concatenate(slabs, 1), smv[level, tap])
            total = term if total is None else total + term
        return total

    def conv(xc, level, image, row, rows):
        return product(
            [
                [xc[image, row + tap : row + tap + rows, slab].reshape(-1, 128) for slab in range(6)]
                for tap in range(3)
            ],
            level,
        )

    def conv_two(image, row):
        values = conv(xc2, 0, image, row, 2)
        cv2[image, row * 256 : row * 256 + 512, :] = values
        tally(0, image, values)

    def conv_five():
        values = product(
            [[xc5[:, tap, slab].reshape(64, 128) for slab in range(6)] for tap in range(3)], 3
        )
        cv5[...] = values
        for image in range(IMAGES):
            tally(3, image, values[32 * image : 32 * image + 32])

    def conv_four():
        for image in range(IMAGES):
            values = conv(xc4, 2, image, 0, 2)
            cv4[128 * image : 128 * image + 128] = values
            tally(2, image, values)

    for image in range(IMAGES):
        halo_five(image)
    for image in range(IMAGES):
        merge_four(image)
    conv_five()
    for image in range(IMAGES):
        merge_three(image)
    conv_four()
    for image in range(IMAGES):
        merge_middle(image)
    for image in range(IMAGES):
        for row in (2, 4):
            conv_two(image, row)


    def conv_three(row, rows):
        for image in range(IMAGES):
            values = conv(xc3, 1, image, row, rows)
            cv3[image, 128 * row : 128 * (row + rows)] = values
            tally(1, image, values)

    phase("wait_edge3")
    receive(edges3, edges2)
    pl.semaphore_wait(entered.at[1], 3)
    greet(entered.at[2], partner)
    ls3.wait()
    phase("rest2")
    for image in range(IMAGES):
        up = dot(t3[512:768, :], middle(xc4, image, 0, 4))
        put_row(rb3, 8 + image, xc3.at[image, 0], (up[0:128] + r3[0, image].astype(F32)) * keep_top)
        put_row(rb3, 10 + image, xc3.at[image, 5], (up[128:256] + r3[1, image].astype(F32)) * keep_bottom)
    def merge_ends(image):
        both = pair(image, -1, t2[512:1024, :])
        outside = dot(r2[0, image], w2v[...]) + biasv[0:1, :]
        base = 12 + 4 * image
        put_row(rb2, base, xc2.at[image, 0], (both[0:256] + outside) * keep_top)
        put_row(rb2, base + 1, xc2.at[image, 1], both[256:512] + cv2[image, 0:256, :])
        both = pair(image, 3, t2[1024:1536, :])
        outside = dot(r2[1, image], w2v[...]) + biasv[0:1, :]
        put_row(rb2, base + 2, xc2.at[image, 8], both[0:256] + cv2[image, 1792:2048, :])
        put_row(rb2, base + 3, xc2.at[image, 9], (both[256:512] + outside) * keep_bottom)

    conv_three(1, 2)
    for image in range(IMAGES):
        merge_ends(image)
    for image in range(IMAGES):
        for row in (0, 6):
            conv_two(image, row)

    def everyone(source, target, which):
        far = lambda i: min(i, SIDE - i)
        moves = sorted(
            ((j, i, c) for j in range(SIDE) for i in range(SIDE) for c in range(2) if i or j or c),
            key=lambda m: (-far(m[0]) - far(m[1]), m),
        )
        along = [2 * lax.rem(x + i, SIDE) for i in range(SIDE)]
        across = [2 * SIDE * lax.rem(y + j, SIDE) for j in range(SIDE)]
        cores = [core, 1 - core]
        return [
            pltpu.make_async_remote_copy(
                src_ref=source,
                dst_ref=target.at[slot],
                send_sem=all_send.at[which],
                recv_sem=all_recv.at[which],
                device_id=(batch, across[j] + along[i] + cores[c]),
                device_id_type=MESH,
            )
            for slot, (j, i, c) in enumerate(moves)
        ]

    phase("encodeA")
    sendA[...] = jnp.concatenate(
        [encode(stats.at[0]), encode(stats.at[2]), encode(stats.at[3]), jnp.zeros((1, 128), F32)], 0
    )
    pl.semaphore_wait(entered.at[2], 1)
    for copy in everyone(sendA, recvA, 0):
        copy.start()

    phase("conv3")
    for image in range(IMAGES):
        values = product(
            [
                [
                    jnp.concatenate([xc3[image, row + tap, slab] for row in (0, 3)], 0)
                    for slab in range(6)
                ]
                for tap in range(3)
            ],
            1,
        )
        cv3[image, 0:128] = values[0:128]
        cv3[image, 384:512] = values[128:256]
        tally(1, image, values)

    phase("encodeB")
    sendB[...] = encode(stats.at[1])
    for copy in everyone(sendB, recvB, 1):
        copy.start()

    lg.wait()
    lsh.wait()
    norms[0:1, :] = gainv[1:2, :]
    norms[1:2, :] = shiftv[1:2, :]
    def finish(level, totals):
        affine = affine_of(level, strips, totals, gainv[level : level + 1], shiftv[level : level + 1])
        for image, terms in enumerate(affine):
            if level == 0 and image == 0:

                @pl.loop(0, 4)
                def _(rows):
                    values = normalized(cv2[0, pl.ds(rows * 512, 512), :], terms)
                    outs[0][0, pl.ds(rows * 2, 2)] = values.reshape(2, 256, 256)

            elif level == 0:
                norms[2:3, :], norms[3:4, :] = terms
            else:
                if level == 2:
                    values = cv4[128 * image : 128 * image + 128]
                else:
                    values = cv5[32 * image : 32 * image + 32]
                outs[level][image] = normalized(values, terms).reshape(
                    STRIP[level], COLS[level], 256
                )

    phase("wait_A")
    pltpu.make_async_copy(recvA, recvA, all_recv.at[0]).wait()
    phase("normA")
    totals = sendA[...] + jnp.sum(recvA[...], axis=0)
    finish(0, totals[0:1])
    finish(2, totals[1:2])
    finish(3, totals[2:3])

    phase("wait_sends")
    @pl.when(has_above)
    def _():
        for pair_of in (edges5, edges4, edges3, edges2):
            pair_of[0].wait_send()

    @pl.when(has_below)
    def _():
        for pair_of in (edges5, edges4, edges3, edges2):
            pair_of[1].wait_send()

    pltpu.make_async_copy(recvA, recvA, all_send.at[0]).wait()
    pltpu.make_async_copy(recvB, recvB, all_send.at[1]).wait()
    phase("wait_B")
    pltpu.make_async_copy(recvB, recvB, all_recv.at[1]).wait()
    phase("normB")
    outs[4][...] = sendB[...] + jnp.sum(recvB[...], axis=0)
    phase(None)


def write_out(
    strips, in2, in4, in5, values, totals, norms, values2, out2, out3, out4, out5, made2, made3, sems
):
    pairs = [(in2, out2.at[pl.ds(0, 1)]), (in4, out4), (in5, out5)]
    pairs += [(made2.at[pl.ds(4 * j, 4)], out2.at[1, pl.ds(4 * j, 4)]) for j in range(2)]
    pairs += [(made3, out3)]
    copies = [pltpu.make_async_copy(*pair, sems.at[k]) for k, pair in enumerate(pairs)]
    for copy in copies[:3]:
        copy.start()
    terms = (norms[2:3, :], norms[3:4, :])
    for j in range(2):
        rows = normalized(values2[1, 1024 * j : 1024 * j + 1024, :], terms)
        made2[4 * j : 4 * j + 4] = rows.reshape(4, COLS[0], CHANNELS)
        copies[3 + j].start()
    affine = affine_of(1, strips, totals[...], norms[0:1, :], norms[1:2, :])
    for image, terms in enumerate(affine):
        made3[image] = normalized(values[image], terms).reshape(STRIP[1], COLS[1], CHANNELS)
    copies[5].start()
    for copy in copies:
        copy.wait()


def solution(mesh):
    strips = mesh.shape["rows"]

    def per_device(*args):
        vmem = pltpu.VMEM
        scratch = [
            vmem((2, 8, 256, 256), BF16), vmem((2, 4, 128, 512), BF16),
            vmem((2, 2, 64, 1024), BF16), vmem((2, 1, 32, 2048), BF16),
            vmem((256, 256), BF16), vmem((512, 256), BF16),
            vmem((1024, 256), BF16), vmem((2048, 256), BF16),
            vmem((4, 256), F32), vmem((4, 3, 768, 256), BF16),
            vmem((4, 256), F32), vmem((4, 256), F32),
            vmem((2, 10, 6, 256, 128), BF16), vmem((2, 6, 6, 128, 128), BF16),
            vmem((2, 4, 6, 64, 128), BF16), vmem((2, 3, 6, 32, 128), BF16),
            vmem((1536, 256), BF16), vmem((768, 256), BF16), vmem((256, 128), BF16),
            vmem((2, 512, 256), F32), vmem((2, 2, 64, 256), F32),
            vmem((2, 32, 256), BF16), vmem((2, 2, 64, 256), BF16), vmem((2, 2, 128, 256), BF16),
            vmem((2, 2, 32, 256), BF16), vmem((2, 2, 64, 256), BF16),
            vmem((2, 2, 128, 256), BF16), vmem((2, 2, 256, 256), BF16),
            vmem((20, 2, 272, 128), F32), vmem((12, 2, 144, 128), F32),
            vmem((8, 2, 80, 128), F32), vmem((6, 2, 48, 128), F32),
            vmem((256, 256), F32), vmem((64, 256), F32),
            vmem((4, 2, 2, 8, 256), F32),
            vmem((4, 128), F32), vmem((1, 128), F32),
            vmem((strips - 1, 4, 128), F32), vmem((strips - 1, 1, 128), F32),
        ]
        results = pl.pallas_call(
            lambda *refs: pl.run_scoped(
                lambda *semaphores: kernel(strips, refs, *semaphores),
                pltpu.SemaphoreType.DMA((15,)),
                pltpu.SemaphoreType.DMA((4, 2)),
                pltpu.SemaphoreType.DMA((4, 2)),
                pltpu.SemaphoreType.DMA((2,)),
                pltpu.SemaphoreType.DMA((2,)),
                pltpu.SemaphoreType.REGULAR((3,)),
            ),
            name="pyramid",
            out_shape=[
                pltpu.VMEM((1 if k == 0 else IMAGES, STRIP[k], COLS[k], CHANNELS), BF16)
                for k in (0, 2, 3)
            ]
            + [
                pltpu.VMEM((IMAGES, STRIP[1] * COLS[1], CHANNELS), F32),
                pltpu.VMEM((1, 128), F32),
                pltpu.VMEM((4, CHANNELS), F32),
                pltpu.VMEM((IMAGES, STRIP[0] * COLS[0], CHANNELS), F32),
            ],
            in_specs=[pl.BlockSpec(memory_space=pltpu.HBM)] * 12,
            out_specs=[pl.BlockSpec(memory_space=pltpu.VMEM)] * 7,
            scratch_shapes=scratch,
            compiler_params=pltpu.CompilerParams(
                collective_id=0, has_side_effects=True, vmem_limit_bytes=48 << 20
            ),
            cost_estimate=pl.CostEstimate(
                flops=7_430_000_000, bytes_accessed=13_300_000, transcendentals=0
            ),
        )(*(pltpu.with_memory_space_constraint(a, pltpu.HBM) for a in args))
        return tuple(
            pl.pallas_call(
                lambda *refs: pl.run_scoped(
                    lambda sems: write_out(strips, *refs, sems), pltpu.SemaphoreType.DMA((6,))
                ),
                name="write",
                out_shape=[
                    jax.ShapeDtypeStruct((IMAGES, STRIP[k], COLS[k], CHANNELS), BF16)
                    for k in range(4)
                ],
                in_specs=[pl.BlockSpec(memory_space=pltpu.VMEM)] * 7,
                out_specs=[pl.BlockSpec(memory_space=pltpu.HBM)] * 4,
                scratch_shapes=[
                    pltpu.VMEM((STRIP[0], COLS[0], CHANNELS), BF16),
                    pltpu.VMEM((IMAGES, STRIP[1], COLS[1], CHANNELS), BF16),
                ],
                compiler_params=pltpu.CompilerParams(vmem_limit_bytes=8 << 20),
                cost_estimate=pl.CostEstimate(
                    flops=0, bytes_accessed=5_600_000, transcendentals=0
                ),
            )(*(pltpu.with_memory_space_constraint(r, pltpu.VMEM) for r in results))
        )

    rows = P("batch", "rows", None, None)
    return jax.shard_map(
        per_device,
        mesh=mesh,
        in_specs=(rows,) * 4 + (P(),) * 8,
        out_specs=(rows,) * 4,
        check_vma=False,
    )
```
